128 devices in a mesh: dp: 32 (over x, y, core), vocab: 4 (over z).
Axes of the slice: x: 4, y: 4, z: 4, core: 2. Of those that a mesh axis runs over, the one named last changes fastest.
Arguments:
- hidden_current: bfloat16 [1024, 4096], P(('dp', 'vocab'))
- hidden_proximal: bfloat16 [1024, 4096], P(('dp', 'vocab'))
- head_current: bfloat16 [4096, 128256], P(None, ('dp', 'vocab'))
- head_proximal: bfloat16 [4096, 128256], P(None, ('dp', 'vocab'))
- targets: int32 [1024], P(('dp', 'vocab')), may hold values from 0 to 128255
- loss_mask: int32 [1024], P(('dp', 'vocab')), may hold values from 0 to 1, as said below
- lengths: int32 [128], P(('dp', 'vocab')), may hold values from 1 to 8
- behavior_logprob: float32 [1024], P(('dp', 'vocab')), may hold values from -14 to -10
- advantages: float32 [1024], P(('dp', 'vocab')), may hold values from -6 to 6
Outputs:
- token_loss: float32 [1024], P(('dp', 'vocab'))
- current_logprob: float32 [1024], P(('dp', 'vocab'))
- stats: float32 [3], replicated
The draws below stay inside these ranges and needn't reach their ends.
Inputs may be any that keep to these rules, and one draw needn't show every extreme that they name: `loss_mask`: 1 at the first position of every sequence's window.
All inputs are finite; a program needn't handle non-finite values.
Results may differ from the reference program's by a relative error of at most 0.0003.
Values may be sent and summed in bfloat16 or wider, within the bound.
No kernel may reach another device: no remote copies, remote signals or barrier semaphores. Data moves between devices by JAX's collectives and lax.ppermute only.
A program may use at most 128 MiB of HBM per device.

```python
import math
import jax
import jax.numpy as jnp
import numpy as np
from jax import lax

D = 4096
VOCAB = 128256
POSITIONS = 8
SEQS = 128
TOKENS = 1024


def hidden_base(key):
    return jax.random.normal(jax.random.fold_in(key, 21), (TOKENS, D), jnp.float32)


def head_base(key):
    return jax.random.normal(jax.random.fold_in(key, 41), (D, VOCAB), jnp.float32) * D ** (-0.5)


def draw_hidden_current(key, part):
    return hidden_base(key).astype(jnp.bfloat16)


def draw_hidden_proximal(key, part):
    noise = jax.random.normal(jax.random.fold_in(key, 22), (TOKENS, D), jnp.float32)
    return (hidden_base(key) + 0.15 * noise).astype(jnp.bfloat16)


def draw_head_current(key, part):
    return head_base(key).astype(jnp.bfloat16)


def draw_head_proximal(key, part):
    spread = 0.15
    noise = jax.random.normal(jax.random.fold_in(key, 42), (D, VOCAB), jnp.float32) * D ** (-0.5)
    return (head_base(key) + spread * noise).astype(jnp.bfloat16)


def draw_loss_mask(key, part):
    coin = jax.random.randint(jax.random.fold_in(key, 51), (TOKENS,), 0, 4)
    place = jnp.arange(TOKENS, dtype=jnp.int32) % POSITIONS
    return jnp.where((place == 0) | (coin < 3), 1, 0).astype(jnp.int32)


def touch_ends(values, key, low, high):
    longest = values.shape.index(max(values.shape))
    spots = []
    for shift in (0, 1):
        where = [jax.random.randint(jax.random.fold_in(key, axis), (), 0, length) for axis, length in enumerate(values.shape)]
        where[longest] = (where[longest] + shift) % values.shape[longest]
        spots.append(tuple(where))
    return values.at[spots[0]].set(low).at[spots[1]].set(high)


def levels(key, shape, shards, low, top_value):
    gain, own = 1.0, jax.random.fold_in(key, 6)
    for axis_at, shards_of in shards:
        steps = jnp.exp(jax.random.uniform(jax.random.fold_in(own, axis_at), (shards_of,), jnp.float32, low / len(shards), top_value / len(shards)))
        gain = gain * jnp.repeat(steps, shape[axis_at] // shards_of).reshape([-1 if axis == axis_at else 1 for axis in range(len(shape))])
    return gain


def ranked_wide(key, extent, count, slope):
    weights = [min(1 << octave, count + 1 - (1 << octave)) * (1 << 20) // math.isqrt((1 << octave) ** slope) + 1 for octave in range((count + 1).bit_length()) if 1 << octave <= count]
    scale = 1 + sum(weights) // (1 << 30)
    listing = np.cumsum(np.array([max(1, weight // scale) for weight in weights]))
    ticket = jax.random.randint(jax.random.fold_in(key, 1), extent, 0, int(listing[len(weights) - 1]))
    start = jnp.left_shift(1, jnp.searchsorted(jnp.asarray(listing, jnp.int32), ticket, side="right").astype(jnp.int32))
    rank = start - 1 + jax.random.randint(jax.random.fold_in(key, 4), extent, 0, 1 << 30) % jnp.minimum(start, count + 1 - start)
    return jax.random.permutation(jax.random.fold_in(key, 2), count)[rank].astype(jnp.int32)


def centred(key, shape, deviation, reach, pieces=(), kind=jnp.bfloat16):
    result = deviation * jax.random.normal(key, shape, jnp.float32)
    if pieces:
        result = result * levels(key, shape, pieces, -0.22, 0.18)
    return jnp.clip(result, -reach, reach).astype(kind)


def setup_inputs(seed: int = 0) -> dict:
    arg_keys = jax.random.split(jax.random.key(seed), 10)
    return {
        "hidden_current": draw_hidden_current(jax.random.fold_in(arg_keys[9], 71), 0),
        "hidden_proximal": draw_hidden_proximal(jax.random.fold_in(arg_keys[9], 71), 0),
        "head_current": draw_head_current(jax.random.fold_in(arg_keys[9], 71), 0),
        "head_proximal": draw_head_proximal(jax.random.fold_in(arg_keys[9], 71), 0),
        "targets": touch_ends(ranked_wide(arg_keys[4], (TOKENS,), VOCAB, 2), jax.random.fold_in(arg_keys[4], 3), 0, VOCAB - 1).astype(jnp.int32),
        "loss_mask": draw_loss_mask(jax.random.fold_in(arg_keys[9], 71), 0),
        "lengths": touch_ends(jax.random.randint(arg_keys[6], (SEQS,), 1, POSITIONS + 1), jax.random.fold_in(arg_keys[6], 1), 1, POSITIONS).astype(jnp.int32),
        "behavior_logprob": jnp.clip(-14.0 + 4.0 * jax.random.uniform(arg_keys[7], (TOKENS,), jnp.float32) ** levels(arg_keys[7], (TOKENS,), ((0, 128),), -0.2, 0.2), -14.0, -10.0),
        "advantages": centred(arg_keys[8], (TOKENS,), 1.0, 6.0, ((0, 128),), jnp.float32),
    }


CLIP_EPS = 0.2
WEIGHT_CAP = 5.0


def column_stats(logits, wanted, first_col, with_entropy):
    peak = jnp.max(logits, axis=1)
    weights = jnp.exp(logits - peak[:, None])
    total = jnp.sum(weights, axis=1)
    columns = first_col + lax.broadcasted_iota(jnp.int32, logits.shape, 1)
    picked = jnp.sum(jnp.where(columns == wanted[:, None], logits, jnp.float32(0.0)), axis=1)
    if with_entropy:
        moment = jnp.sum(weights * logits, axis=1)
        return [peak, total, moment, picked]
    return [peak, total, picked]


def token_terms(logp_current, logp_proximal, entropy, advantages, behavior, live):
    ratio = jnp.exp(logp_current - logp_proximal)
    clipped = jnp.clip(ratio, 1.0 - CLIP_EPS, 1.0 + CLIP_EPS)
    surrogate = jnp.maximum(-advantages * ratio, -advantages * clipped)
    weight = jnp.minimum(jnp.exp(logp_proximal - behavior), WEIGHT_CAP)
    return surrogate * weight * live, weight * live, entropy * live


def reference(hidden_current, hidden_proximal, head_current, head_proximal, targets, loss_mask, lengths, behavior_logprob, advantages):
    blocks = 16
    width = VOCAB // blocks

    def one_block(index):
        first_col = (index * width).astype(jnp.int32)
        part_c = lax.dynamic_slice_in_dim(head_current, first_col, width, 1)
        part_p = lax.dynamic_slice_in_dim(head_proximal, first_col, width, 1)
        logits_c = jnp.dot(hidden_current, part_c, preferred_element_type=jnp.float32)
        logits_p = jnp.dot(hidden_proximal, part_p, preferred_element_type=jnp.float32)
        return tuple(column_stats(logits_c, targets, first_col, True) + column_stats(logits_p, targets, first_col, False))

    parts = lax.map(one_block, jnp.arange(blocks, dtype=jnp.int32))
    peak_c = jnp.max(parts[0], axis=0)
    scale_c = jnp.exp(parts[0] - peak_c[None, :])
    total_c = jnp.sum(parts[1] * scale_c, axis=0)
    moment_c = jnp.sum(parts[2] * scale_c, axis=0)
    picked_c = jnp.sum(parts[3], axis=0)
    peak_p = jnp.max(parts[4], axis=0)
    total_p = jnp.sum(parts[5] * jnp.exp(parts[4] - peak_p[None, :]), axis=0)
    picked_p = jnp.sum(parts[6], axis=0)
    lse_c = peak_c + jnp.log(total_c)
    logp_c = picked_c - lse_c
    entropy = lse_c - moment_c / total_c
    logp_p = picked_p - (peak_p + jnp.log(total_p))
    place = jnp.arange(TOKENS, dtype=jnp.int32) % POSITIONS
    owner = jnp.arange(TOKENS, dtype=jnp.int32) // POSITIONS
    live = ((place < lengths[owner]) & (loss_mask == 1)).astype(jnp.float32)
    loss_t, weight_t, ent_t = token_terms(logp_c, logp_p, entropy, advantages, behavior_logprob, live)
    count = jnp.sum(live)
    stats = jnp.stack([jnp.sum(loss_t) / count, jnp.sum(weight_t) / count, jnp.sum(ent_t) / count])
    return loss_t, logp_c, stats
```

```python
import functools

import jax
import jax.numpy as jnp
from jax import lax
from jax.experimental import pallas as pl
from jax.experimental.pallas import tpu as pltpu
from jax.sharding import Mesh
from jax.sharding import PartitionSpec as P

POSITIONS = 8
AXES = ("dp_0", "dp_1", "dp_2", "vocab")
SIZES = (4, 4, 2, 4)
CLIP_EPS = 0.2
WEIGHT_CAP = 5.0
EXTRA = 128
SLICES = 3


def flip(coordinate, bit):
    return coordinate ^ 1 if bit == 0 else 3 - coordinate


def index_of(x, y, c, z):
    return ((x * 4 + y) * 2 + c) * 4 + z


def swap_pairs(dim, late):
    pairs = []
    for x in range(4):
        for y in range(4):
            for c in range(2):
                for z in range(4):
                    bit = (c + late) % 2
                    to = [x, y, z]
                    to[dim] = flip(to[dim], bit)
                    pairs.append((index_of(x, y, c, z), index_of(to[0], to[1], c, to[2])))
    return pairs


def core_pairs():
    return [(k, k ^ 4) for k in range(128)]


def swap(value, dim, late):
    return lax.ppermute(value, AXES, swap_pairs(dim, late))


def swap_core(value):
    return lax.ppermute(value, AXES, core_pairs())


def three_parts(value):
    high = lax.reduce_precision(value, 8, 7)
    middle = lax.reduce_precision(value - high, 8, 7)
    return [high, middle, value - high - middle]


def head_kernel(rows_of, scal, sel, *refs):
    pieces, refs = refs[:10], refs[10:]
    heads, (stats_out, extra_out, hidden, w0, w1, sem) = refs[:4], refs[4:]
    core, late = scal[0], scal[1]

    @pl.when(core == 0)
    def _():
        pltpu.make_async_copy(heads[0], w0, sem.at[0]).start()
        pltpu.make_async_copy(heads[2], w1, sem.at[1]).start()

    @pl.when(core == 1)
    def _():
        pltpu.make_async_copy(heads[1], w0, sem.at[0]).start()
        pltpu.make_async_copy(heads[3], w1, sem.at[1]).start()

    early, rest = pieces[0], pieces[1:]
    width = early.shape[1] // SLICES
    depth = hidden.shape[1]
    for s in range(SLICES):
        first = s * width
        real = min(width, depth - first)
        for at, relative in enumerate(rows_of[s]):
            if at == 0:
                block = early[:, first : first + real]
            elif at == 1:
                block = rest[s][:, :real]
            elif at < 4:
                block = rest[3 + s][(at - 2) * 128 : (at - 1) * 128, :real]
            else:
                block = rest[6 + s][(at - 4) * 128 : (at - 3) * 128, :real]
            group = relative ^ late
            start = pl.multiple_of(group * 128, 128)
            hidden[pl.ds(start, 128), first : first + real] = block
            if s == SLICES - 1:
                if at == 0:
                    more = early[:, depth:]
                elif at == 1:
                    more = rest[s][:, real:]
                elif at < 4:
                    more = rest[3 + s][(at - 2) * 128 : (at - 1) * 128, real:]
                else:
                    more = rest[6 + s][(at - 4) * 128 : (at - 3) * 128, real:]
                extra_out[:, pl.ds(start, 128)] = lax.dot_general(
                    sel[...], more, (((1,), (1,)), ((), ())), preferred_element_type=jnp.float32
                )

    for h, weights in enumerate((w0, w1)):
        pltpu.make_async_copy(heads[2 * h], weights, sem.at[h]).wait()
        first_col = scal[2 + h]

        def tile(g, carry, weights=weights, first_col=first_col, h=h):
            start = pl.multiple_of(g * 256, 256)
            logits = lax.dot_general(
                weights[...],
                hidden[pl.ds(start, 256), :],
                (((1,), (1,)), ((), ())),
                preferred_element_type=jnp.float32,
            )
            wanted = extra_out[0:1, pl.ds(start, 256)].astype(jnp.int32) - first_col
            peak = jnp.max(logits, axis=0, keepdims=True)
            if h:
                peak = jnp.maximum(peak, stats_out[0:1, pl.ds(start, 256)])
            powers = jnp.exp(logits - peak)
            total = jnp.sum(powers, axis=0, keepdims=True)
            moment = jnp.sum(powers * logits, axis=0, keepdims=True)
            row = lax.broadcasted_iota(jnp.int32, logits.shape, 0)
            picked = jnp.sum(jnp.where(row == wanted, logits, 0.0), axis=0, keepdims=True)
            if h:
                scale = jnp.exp(stats_out[0:1, pl.ds(start, 256)] - peak)
                total = total + stats_out[1:2, pl.ds(start, 256)] * scale
                moment = moment + stats_out[2:3, pl.ds(start, 256)] * scale
                picked = picked + stats_out[3:4, pl.ds(start, 256)]
            stats_out[0:1, pl.ds(start, 256)] = peak
            stats_out[1:2, pl.ds(start, 256)] = total
            stats_out[2:3, pl.ds(start, 256)] = moment
            stats_out[3:4, pl.ds(start, 256)] = picked
            return carry

        lax.fori_loop(0, hidden.shape[0] // 256, tile, 0)


def head_stats(scal, sel, pieces, heads, tokens, depth):
    columns = heads[0].shape[0]
    rows_of = (
        (0, 1, 2, 3, 4, 5, 6, 7),
        (0, 2, 4, 6, 1, 3, 5, 7),
        (0, 4, 1, 5, 2, 6, 3, 7),
    )
    vmem = pl.BlockSpec(memory_space=pltpu.VMEM)
    return pl.pallas_call(
        functools.partial(head_kernel, rows_of),
        out_shape=(
            jax.ShapeDtypeStruct((4, tokens), jnp.float32),
            jax.ShapeDtypeStruct((8, tokens), jnp.float32),
        ),
        in_specs=[pl.BlockSpec(memory_space=pltpu.SMEM), vmem]
        + [vmem] * 10
        + [pl.BlockSpec(memory_space=pl.ANY)] * 4,
        out_specs=(vmem, vmem),
        scratch_shapes=[
            pltpu.VMEM((tokens, depth), jnp.bfloat16),
            pltpu.VMEM((columns, depth), jnp.bfloat16),
            pltpu.VMEM((columns, depth), jnp.bfloat16),
            pltpu.SemaphoreType.DMA((2,)),
        ],
        compiler_params=pltpu.CompilerParams(vmem_limit_bytes=40 * 1024 * 1024),
        cost_estimate=pl.CostEstimate(
            flops=4 * tokens * columns * depth, bytes_accessed=4 * columns * depth, transcendentals=2 * tokens * columns
        ),
        name="head_stats",
    )(scal, sel, *pieces, *heads)


def merge(a, b):
    peak = jnp.maximum(a[0:1], b[0:1])
    fa, fb = jnp.exp(a[0:1] - peak), jnp.exp(b[0:1] - peak)
    return jnp.concatenate([peak, a[1:3] * fa + b[1:3] * fb, a[3:4] + b[3:4]], axis=0)


def token_terms(logp_current, logp_proximal, entropy, advantages, behavior, live):
    ratio = jnp.exp(logp_current - logp_proximal)
    clipped = jnp.clip(ratio, 1.0 - CLIP_EPS, 1.0 + CLIP_EPS)
    surrogate = jnp.maximum(-advantages * ratio, -advantages * clipped)
    weight = jnp.minimum(jnp.exp(logp_proximal - behavior), WEIGHT_CAP)
    return (surrogate * weight * live, weight * live, entropy * live)


def either(first, a, b):
    return jnp.where(first, jnp.concatenate([a, b], axis=0), jnp.concatenate([b, a], axis=0))


def local(
    hidden_current,
    hidden_proximal,
    head_current,
    head_proximal,
    targets,
    loss_mask,
    lengths,
    behavior_logprob,
    advantages,
):
    own, depth = hidden_current.shape
    columns = head_current.shape[1]
    tokens = own * 128
    me = [lax.axis_index(a) for a in AXES]
    x, y, core, z = me
    device = index_of(x, y, core, z)
    low = [(v & 1) ^ (v >> 1) for v in (x, y, z)]
    high = [v >> 1 for v in (x, y, z)]
    early_bits = [jnp.where(core == 0, a, b) for a, b in zip(low, high)]
    late_bits = [jnp.where(core == 0, b, a) for a, b in zip(low, high)]
    early_at = early_bits[0] + 2 * early_bits[1] + 4 * early_bits[2]
    late_at = late_bits[0] + 2 * late_bits[1] + 4 * late_bits[2]

    heads_c, heads_p = head_current.T, head_proximal.T
    other_c = swap_core(heads_c)
    other_p = swap_core(heads_p)

    place = lax.broadcasted_iota(jnp.int32, (lengths.shape[0], POSITIONS), 1)
    live = ((place < lengths[:, None]).reshape(-1) & (loss_mask == 1)).astype(jnp.float32)
    lines = [(targets & 255).astype(jnp.float32), ((targets >> 8) & 255).astype(jnp.float32)]
    lines += [(targets >> 16).astype(jnp.float32)]
    lines += three_parts(advantages) + three_parts(behavior_logprob) + [live]
    extra = jnp.stack(lines, axis=1).astype(jnp.bfloat16)
    extra = jnp.pad(extra, ((0, 0), (0, EXTRA - extra.shape[1])))

    first = core == 0
    keep = jnp.concatenate([jnp.where(first, hidden_current, hidden_proximal), extra], axis=1)
    give = jnp.concatenate([jnp.where(first, hidden_proximal, hidden_current), extra], axis=1)
    block = either(first, keep, swap_core(give))
    for dim in range(3):
        block = either(early_bits[dim] == 0, block, swap(block, dim, 0))

    width = (depth + EXTRA) // SLICES
    sent = [block[:, s * width : (s + 1) * width] for s in range(SLICES)]
    pieces = [block]
    for level in range(3):
        got = [swap(sent[s], (s + level) % 3, 1) for s in range(SLICES)]
        pieces += got
        if level < 2:
            sent = [jnp.concatenate([a, b], axis=0) for a, b in zip(sent, got)]

    weights = [(0, 0, 1.0), (0, 1, 256.0), (0, 2, 65536.0)]
    weights += [(1, 3 + k, 1.0) for k in range(3)] + [(2, 6 + k, 1.0) for k in range(3)] + [(3, 9, 1.0)]
    line = lax.broadcasted_iota(jnp.int32, (8, EXTRA), 0)
    lane = lax.broadcasted_iota(jnp.int32, (8, EXTRA), 1)
    sel = jnp.zeros((8, EXTRA), jnp.float32)
    for a, b, w in weights:
        sel = jnp.where((line == a) & (lane == b), w, sel)
    scal = jnp.stack([core, late_at, device * columns, (device ^ 4) * columns]).astype(jnp.int32)
    stats, extras = head_stats(
        scal, sel.astype(jnp.bfloat16), pieces, [heads_c, heads_p, other_c, other_p], tokens, depth
    )
    for late in (0, 1):
        for dim in range(3):
            stats = merge(stats, swap(stats, dim, late))

    lse = stats[0:1] + jnp.log(stats[1:2])
    logp = stats[3:4] - lse
    entropy = lse - stats[2:3] / stats[1:2]
    mine = jnp.concatenate([logp, entropy], axis=0)
    other = swap_core(mine).reshape(2, 8, 8, 16).swapaxes(1, 2).reshape(2, tokens)
    logp_c = jnp.where(first, mine[0], other[0])
    logp_p = jnp.where(first, other[0], mine[0])
    entropy = jnp.where(first, mine[1], other[1])
    adv, behavior, live_all = extras[1], extras[2], extras[3]
    loss_all, weight_all, ent_all = token_terms(logp_c, logp_p, entropy, adv, behavior, live_all)
    count = jnp.sum(live_all)
    summary = jnp.stack([jnp.sum(loss_all) / count, jnp.sum(weight_all) / count, jnp.sum(ent_all) / count])
    row_start = late_at * 128 + early_at * 16 + core * 8

    def own_rows(values):
        return lax.dynamic_slice_in_dim(values, row_start, own)

    return (own_rows(loss_all), own_rows(logp_c), summary)


def solution(mesh):
    torus = Mesh(mesh.devices.reshape(4, 4, 2, mesh.shape["vocab"]), AXES)
    spec = P(AXES)
    return jax.shard_map(
        local,
        mesh=torus,
        in_specs=(P(AXES, None), P(AXES, None), P(None, AXES), P(None, AXES)) + (spec,) * 5,
        out_specs=(spec, spec, P()),
        check_vma=False,
    )
```

```python
import functools

import jax
import jax.numpy as jnp
import numpy as np
from jax import lax
from jax.experimental import pallas as pl
from jax.experimental.pallas import tpu as pltpu
from jax.sharding import Mesh
from jax.sharding import PartitionSpec as P

POSITIONS = 8
AXES = ("dp_0", "dp_1", "dp_2", "vocab")
SIZES = (4, 4, 2, 4)
CLIP_EPS = 0.2
WEIGHT_CAP = 5.0
EXTRA = 128
LATE_BIT = ((1, 0, 0), (0, 1, 1))


def flip(coordinate, bit):
    return coordinate ^ 1 if bit == 0 else 3 - coordinate


def index_of(x, y, c, z):
    return ((x * 4 + y) * 2 + c) * 4 + z


def swap_pairs(dim, late):
    pairs = []
    for x in range(4):
        for y in range(4):
            for c in range(2):
                for z in range(4):
                    bit = LATE_BIT[c][dim] if late else 1 - LATE_BIT[c][dim]
                    to = [x, y, z]
                    to[dim] = flip(to[dim], bit)
                    pairs.append((index_of(x, y, c, z), index_of(to[0], to[1], c, to[2])))
    return pairs


def swap(value, dim, late):
    return lax.ppermute(value, AXES, swap_pairs(dim, late))


def swap_core(value):
    return lax.ppermute(value, AXES, [(k, k ^ 4) for k in range(128)])


VMEM = pl.BlockSpec(memory_space=pltpu.VMEM)
SMEM = pl.BlockSpec(memory_space=pltpu.SMEM)
HBM = pl.BlockSpec(memory_space=pltpu.HBM)
NT = (((1,), (1,)), ((), ()))
SMALL = pltpu.CompilerParams(vmem_limit_bytes=4 * 1024 * 1024)


def column_of(line):
    rows = lax.broadcasted_iota(jnp.int32, (8, 8), 0)
    lanes = lax.broadcasted_iota(jnp.int32, (8, 8), 1)
    spread = jnp.broadcast_to(line, (8, 8))
    return jnp.sum(jnp.where(rows == lanes, spread, 0.0), axis=1, keepdims=True)


def three_parts(value):
    high = value.astype(jnp.bfloat16).astype(jnp.float32)
    middle = (value - high).astype(jnp.bfloat16).astype(jnp.float32)
    return [high, middle, value - high - middle]


def extra_kernel(lines, extra):
    lane = lax.broadcasted_iota(jnp.int32, extra.shape, 1)
    table = jnp.zeros(extra.shape, jnp.float32)
    at = 0
    for k in range(lines.shape[0]):
        line = lines[k : k + 1, :]
        for part in three_parts(line) if k in (3, 4) else [line]:
            table = jnp.where(lane == at, column_of(part), table)
            at += 1
    extra[...] = table.astype(jnp.bfloat16)


def load_kernel(scal, hc, hp, oc, op, w0, w1, sem):
    for core, pair in enumerate(((hc, oc), (hp, op))):

        @pl.when(scal[0] == core)
        def _(pair=pair):
            pltpu.make_async_copy(pair[0], w0, sem.at[0]).start()
            pltpu.make_async_copy(pair[1], w1, sem.at[1]).start()

    pltpu.make_async_copy(hc, w0, sem.at[0]).wait()
    pltpu.make_async_copy(oc, w1, sem.at[1]).wait()


def chunk_stats(scal, w0, w1, sel, pieces, hidden, out):
    depth = hidden.shape[1]
    at = 0
    for piece in pieces:
        rows = piece.shape[0]
        hidden[at : at + rows, :] = piece[:, :depth]
        out[4:8, at : at + rows] = lax.dot_general(
            sel[...], piece[:, depth:], NT, preferred_element_type=jnp.float32
        )[0:4]
        at += rows
    target = out[4:5, :].astype(jnp.int32)
    before = None
    for h, weights in enumerate((w0, w1)):
        logits = lax.dot_general(
            weights[...], hidden[...], NT, preferred_element_type=jnp.float32
        )
        wanted = target - scal[2 + h]
        peak = jnp.max(logits, axis=0, keepdims=True)
        if before is not None:
            peak = jnp.maximum(peak, before[0])
        powers = jnp.exp(logits - peak)
        total = jnp.sum(powers, axis=0, keepdims=True)
        moment = jnp.sum(powers * logits, axis=0, keepdims=True)
        row = lax.broadcasted_iota(jnp.int32, logits.shape, 0)
        picked = jnp.sum(jnp.where(row == wanted, logits, 0.0), axis=0, keepdims=True)
        if before is not None:
            scale = jnp.exp(before[0] - peak)
            total = total + before[1] * scale
            moment = moment + before[2] * scale
            picked = picked + before[3]
        before = (peak, total, moment, picked)
    for k in range(4):
        out[k : k + 1, :] = before[k]


def chunk_kernel(scal, w0, w1, sel, *refs):
    chunk_stats(scal, w0, w1, sel, refs[:-2], refs[-1], refs[-2])


def last_kernel(groups, scal, w0, w1, sel, *refs):
    done, pieces = refs[:3], refs[3:-4]
    stats, extras, hidden, mine = refs[-4:]
    chunk_stats(scal, w0, w1, sel, pieces, hidden, mine)
    for chunk, pair in zip((*done, mine), groups):
        for k, relative in enumerate(pair):
            lanes = pl.ds(pl.multiple_of((relative ^ scal[1]) * 128, 128), 128)
            stats[:, lanes] = chunk[0:4, k * 128 : (k + 1) * 128]
            extras[:, lanes] = chunk[4:8, k * 128 : (k + 1) * 128]


def final_kernel(scal, mine, other, extras, loss_out, logp_out, summary_out, lines):
    first = scal[0] == 0
    logp_c = jnp.where(first, mine[0:1, :], other[0:1, :])
    logp_p = jnp.where(first, other[0:1, :], mine[0:1, :])
    entropy = jnp.where(first, mine[1:2, :], other[1:2, :])
    live = extras[3:4, :]
    loss, weight, ent = token_terms(logp_c, logp_p, entropy, extras[1:2, :], extras[2:3, :], live)
    count = jnp.sum(live, axis=1, keepdims=True)
    lane = lax.broadcasted_iota(jnp.int32, (1, 3), 1)
    summary = jnp.where(lane == 0, jnp.sum(loss, axis=1, keepdims=True), 0.0)
    summary = jnp.where(lane == 1, jnp.sum(weight, axis=1, keepdims=True), summary)
    summary = jnp.where(lane == 2, jnp.sum(ent, axis=1, keepdims=True), summary)
    summary_out[...] = summary / count
    lines[0:1, :] = loss
    lines[1:2, :] = logp_c
    block = lines[:, pl.ds(pl.multiple_of(scal[1] * 128, 128), 128)]
    block = pltpu.roll(block, scal[4], 1)
    loss_out[...] = block[0:1, 0:8]
    logp_out[...] = block[1:2, 0:8]


def merge(a, b):
    peak = jnp.maximum(a[0:1], b[0:1])
    fa, fb = jnp.exp(a[0:1] - peak), jnp.exp(b[0:1] - peak)
    return jnp.concatenate([peak, a[1:3] * fa + b[1:3] * fb, a[3:4] + b[3:4]], axis=0)


def token_terms(logp_current, logp_proximal, entropy, advantages, behavior, live):
    ratio = jnp.exp(logp_current - logp_proximal)
    clipped = jnp.clip(ratio, 1.0 - CLIP_EPS, 1.0 + CLIP_EPS)
    surrogate = jnp.maximum(-advantages * ratio, -advantages * clipped)
    weight = jnp.minimum(jnp.exp(logp_proximal - behavior), WEIGHT_CAP)
    return (surrogate * weight * live, weight * live, entropy * live)


def either(first, a, b):
    return jnp.where(first, jnp.concatenate([a, b], axis=0), jnp.concatenate([b, a], axis=0))


def local(
    hidden_current,
    hidden_proximal,
    head_current,
    head_proximal,
    targets,
    loss_mask,
    lengths,
    behavior_logprob,
    advantages,
):
    f32, bf16 = jnp.float32, jnp.bfloat16
    own, depth = hidden_current.shape
    columns = head_current.shape[1]
    tokens = own * 128
    x, y, core, z = [lax.axis_index(a) for a in AXES]
    device = index_of(x, y, core, z)
    first = core == 0
    low = [(v & 1) ^ (v >> 1) for v in (x, y, z)]
    high = [v >> 1 for v in (x, y, z)]
    early_bits, late_bits = [], []
    for dim in range(3):
        pair = (low[dim], high[dim]) if LATE_BIT[0][dim] else (high[dim], low[dim])
        early_bits.append(jnp.where(first, pair[0], pair[1]))
        late_bits.append(jnp.where(first, pair[1], pair[0]))
    early_at = early_bits[0] + 2 * early_bits[1] + 4 * early_bits[2]
    late_at = late_bits[0] + 2 * late_bits[1] + 4 * late_bits[2]
    back = (128 - early_at * 16 - core * 8) % 128
    scal = jnp.stack([core, late_at, device * columns, (device ^ 4) * columns, back]).astype(jnp.int32)

    place = lax.broadcasted_iota(jnp.int32, (lengths.shape[0], POSITIONS), 1)
    live = (place < lengths[:, None]).reshape(-1) & (loss_mask == 1)
    lines = [targets & 255, (targets >> 8) & 255, targets >> 16, advantages, behavior_logprob, live]
    extra = pl.pallas_call(
        extra_kernel,
        out_shape=jax.ShapeDtypeStruct((own, EXTRA), bf16),
        in_specs=[VMEM],
        out_specs=VMEM,
        compiler_params=SMALL,
        name="extra",
    )(jnp.stack([v.astype(f32) for v in lines]))
    keep = jnp.concatenate([jnp.where(first, hidden_current, hidden_proximal), extra], axis=1)
    give = jnp.concatenate([jnp.where(first, hidden_proximal, hidden_current), extra], axis=1)
    block = either(first, keep, swap_core(give))
    heads_c, heads_p, block = lax.optimization_barrier((head_current.T, head_proximal.T, block))
    other_c = swap_core(heads_c)
    other_p = swap_core(heads_p)
    for dim in range(3):
        block = either(early_bits[dim] == 0, block, swap(block, dim, 0))

    group = {0: block}
    for dim in range(3):
        group[1 << dim] = swap(block, dim, 1)
    weights = [(0, 0, 1.0), (0, 1, 256.0), (0, 2, 65536.0)]
    weights += [(1, 3 + k, 1.0) for k in range(3)]
    weights += [(2, 6 + k, 1.0) for k in range(3)] + [(3, 9, 1.0)]
    table = np.zeros((8, EXTRA), np.float32)
    for a, b, w in weights:
        table[a, b] = w
    sel = jnp.asarray(table, bf16)

    w0, w1 = pl.pallas_call(
        load_kernel,
        out_shape=(jax.ShapeDtypeStruct((columns, depth), bf16),) * 2,
        in_specs=[SMEM] + [HBM] * 4,
        out_specs=(VMEM, VMEM),
        scratch_shapes=[pltpu.SemaphoreType.DMA((2,))],
        compiler_params=pltpu.CompilerParams(vmem_limit_bytes=34 * 1024 * 1024),
        cost_estimate=pl.CostEstimate(
            flops=4 * 1024 * 2048 * 256, bytes_accessed=8 * columns * depth, transcendentals=0
        ),
        name="load_heads",
    )(scal, heads_c, heads_p, other_c, other_p)

    cost = pl.CostEstimate(
        flops=4 * 256 * columns * depth,
        bytes_accessed=4 * columns * depth,
        transcendentals=2 * 256 * columns,
    )
    limit = pltpu.CompilerParams(vmem_limit_bytes=24 * 1024 * 1024)
    hidden = pltpu.VMEM((256, depth), bf16)

    def chunk(one, two):
        return pl.pallas_call(
            chunk_kernel,
            out_shape=jax.ShapeDtypeStruct((8, 256), f32),
            in_specs=[SMEM] + [VMEM] * 5,
            out_specs=VMEM,
            scratch_shapes=[hidden],
            compiler_params=limit,
            cost_estimate=cost,
            name="chunk_stats",
        )(scal, w0, w1, sel, one, two)

    groups = ((0, 1), (2, 4), (3, 5), (6, 7))
    w0, w1, group[1] = lax.optimization_barrier((w0, w1, group[1]))
    group[5] = swap(group[1], 2, 1)
    group[3] = swap(group[2], 0, 1)
    group[6] = swap(group[4], 1, 1)
    ready = [chunk(group[a], group[b]) for a, b in groups[:2]]
    *ready, group[5] = lax.optimization_barrier((*ready, group[5]))
    half = 64
    part_one = swap(group[5][:half], 1, 1)
    part_two = swap(group[3][half:], 2, 1)
    ready.append(chunk(group[3], group[5]))
    stats, extras = pl.pallas_call(
        functools.partial(last_kernel, groups),
        out_shape=(jax.ShapeDtypeStruct((4, tokens), f32),) * 2,
        in_specs=[SMEM] + [VMEM] * 9,
        out_specs=(VMEM, VMEM),
        scratch_shapes=[hidden, pltpu.VMEM((8, 256), f32)],
        compiler_params=limit,
        cost_estimate=cost,
        name="last_stats",
    )(scal, w0, w1, sel, *ready, group[6], part_one, part_two)

    for late in (0, 1):
        for dim in range(3):
            stats = merge(stats, swap(stats, dim, late))

    lse = stats[0:1] + jnp.log(stats[1:2])
    mine = jnp.concatenate([stats[3:4] - lse, lse - stats[2:3] / stats[1:2]], axis=0)
    other = swap_core(mine).reshape(2, 8, 8, 16).swapaxes(1, 2).reshape(2, tokens)
    loss, logp, summary = pl.pallas_call(
        final_kernel,
        out_shape=(
            jax.ShapeDtypeStruct((1, own), f32),
            jax.ShapeDtypeStruct((1, own), f32),
            jax.ShapeDtypeStruct((1, 3), f32),
        ),
        in_specs=[SMEM, VMEM, VMEM, VMEM],
        out_specs=(VMEM, VMEM, VMEM),
        scratch_shapes=[pltpu.VMEM((8, tokens), f32)],
        compiler_params=SMALL,
        name="final",
    )(scal, mine, other, extras)
    return (loss.reshape(own), logp.reshape(own), summary.reshape(3))


def solution(mesh):
    torus = Mesh(mesh.devices.reshape(4, 4, 2, mesh.shape["vocab"]), AXES)
    spec = P(AXES)
    return jax.shard_map(
        local,
        mesh=torus,
        in_specs=(P(AXES, None), P(AXES, None), P(None, AXES), P(None, AXES)) + (spec,) * 5,
        out_specs=(spec, spec, P()),
        check_vma=False,
    )
```

```python
import jax
import jax.numpy as jnp
import numpy as np
from jax import lax
from jax.experimental import pallas as pl
from jax.experimental.pallas import tpu as pltpu
from jax.sharding import Mesh
from jax.sharding import PartitionSpec as P

AXES = ("dp_0", "dp_1", "dp_2", "vocab")
SIZES = (4, 4, 2, 4)
CLIP_EPS = 0.2
WEIGHT_CAP = 5.0
EXTRA = 128
LATE_BIT = ((1, 0, 0), (0, 1, 1))


def flip(coordinate, bit):
    return coordinate ^ 1 if bit == 0 else 3 - coordinate


def index_of(x, y, c, z):
    return ((x * 4 + y) * 2 + c) * 4 + z


def swap_pairs(dim, late):
    pairs = []
    for x in range(4):
        for y in range(4):
            for c in range(2):
                for z in range(4):
                    bit = LATE_BIT[c][dim] if late else 1 - LATE_BIT[c][dim]
                    to = [x, y, z]
                    to[dim] = flip(to[dim], bit)
                    pairs.append((index_of(x, y, c, z), index_of(to[0], to[1], c, to[2])))
    return pairs


def swap(value, dim, late):
    return lax.ppermute(value, AXES, swap_pairs(dim, late))


def swap_core(value):
    return lax.ppermute(value, AXES, [(k, k ^ 4) for k in range(128)])


VMEM = pl.BlockSpec(memory_space=pltpu.VMEM)
SMEM = pl.BlockSpec(memory_space=pltpu.SMEM)
HBM = pl.BlockSpec(memory_space=pltpu.HBM)
NT = (((1,), (1,)), ((), ()))
SMALL = pltpu.CompilerParams(vmem_limit_bytes=4 * 1024 * 1024)


def column_of(line):
    rows = lax.broadcasted_iota(jnp.int32, (8, 8), 0)
    lanes = lax.broadcasted_iota(jnp.int32, (8, 8), 1)
    spread = jnp.broadcast_to(line, (8, 8))
    return jnp.sum(jnp.where(rows == lanes, spread, 0.0), axis=1, keepdims=True)


def three_parts(value):
    high = value.astype(jnp.bfloat16).astype(jnp.float32)
    middle = (value - high).astype(jnp.bfloat16).astype(jnp.float32)
    return [high, middle, value - high - middle]


def extra_kernel(lines, extra):
    ids = lines[0:1, :].astype(jnp.int32)
    place = lax.broadcasted_iota(jnp.int32, (1, 8), 1).astype(jnp.float32)
    live = jnp.where((place < lines[2:3, :]) & (lines[1:2, :] == 1.0), 1.0, 0.0)
    values = [v.astype(jnp.float32) for v in (ids & 255, (ids >> 8) & 255, ids >> 16)]
    values += three_parts(lines[3:4, :]) + three_parts(lines[4:5, :]) + [live]
    lane = lax.broadcasted_iota(jnp.int32, extra.shape, 1)
    table = jnp.zeros(extra.shape, jnp.float32)
    for k, value in enumerate(values):
        table = jnp.where(lane == k, column_of(value), table)
    extra[...] = table.astype(jnp.bfloat16)


def load_kernel(scal, for_c, for_p, weights, sem):
    for core, source in enumerate((for_c, for_p)):

        @pl.when(scal[0] == core)
        def _(source=source):
            pltpu.make_async_copy(source, weights, sem.at[0]).start()

    pltpu.make_async_copy(for_c, weights, sem.at[0]).wait()


def chunk_stats(scal, w0, w1, sel, pieces, hidden, out):
    depth = hidden.shape[1]
    at = 0
    for piece in pieces:
        rows = piece.shape[0]
        hidden[at : at + rows, :] = piece[:, :depth]
        out[4:8, at : at + rows] = lax.dot_general(
            sel[...], piece[:, depth:], NT, preferred_element_type=jnp.float32
        )[0:4]
        at += rows
    target = out[4:5, :].astype(jnp.int32)
    before = None
    for h, weights in enumerate((w0, w1)):
        logits = lax.dot_general(
            weights[...], hidden[...], NT, preferred_element_type=jnp.float32
        )
        wanted = target - scal[2 + h]
        peak = jnp.max(logits, axis=0, keepdims=True)
        if before is not None:
            peak = jnp.maximum(peak, before[0])
        powers = jnp.exp(logits - peak)
        total = jnp.sum(powers, axis=0, keepdims=True)
        moment = jnp.sum(powers * logits, axis=0, keepdims=True)
        row = lax.broadcasted_iota(jnp.int32, logits.shape, 0)
        picked = jnp.sum(jnp.where(row == wanted, logits, 0.0), axis=0, keepdims=True)
        if before is not None:
            scale = jnp.exp(before[0] - peak)
            total = total + before[1] * scale
            moment = moment + before[2] * scale
            picked = picked + before[3]
        before = (peak, total, moment, picked)
    for k in range(4):
        out[k : k + 1, :] = before[k]


def chunk_kernel(scal, w0, w1, sel, *refs):
    chunk_stats(scal, w0, w1, sel, refs[:-2], refs[-1], refs[-2])


def last_kernel(scal, w0, w1, sel, *refs):
    (near_one, near_two, third), pieces = refs[:3], refs[3:-4]
    stats, extras, hidden, mine = refs[-4:]
    chunk_stats(scal, w0, w1, sel, pieces, hidden, mine)
    left = lax.broadcasted_iota(jnp.int32, (8, 128), 1) < 64
    blocks = {}
    for k, pair in ((0, (0, 1)), (1, (2, 4))):
        one = near_one[:, k * 128 : (k + 1) * 128]
        two = near_two[:, k * 128 : (k + 1) * 128]
        blocks[pair[0]] = jnp.where(left, one, pltpu.roll(two, 64, 1))
        blocks[pair[1]] = jnp.where(left, pltpu.roll(one, 64, 1), two)
    for chunk, pair in ((third, (3, 5)), (mine, (6, 7))):
        for k in range(2):
            blocks[pair[k]] = chunk[:, k * 128 : (k + 1) * 128]
    for relative, block in blocks.items():
        block = jnp.where(scal[5] == 1, pltpu.roll(block, 64, 1), block)
        lanes = pl.ds(pl.multiple_of((relative ^ scal[1]) * 128, 128), 128)
        stats[:, lanes] = block[0:4]
        extras[:, lanes] = block[4:8]


def final_kernel(scal, mine, other, extras, loss_out, logp_out, summary_out, lines):
    first = scal[0] == 0
    logp_c = jnp.where(first, mine[0:1, :], other[0:1, :])
    logp_p = jnp.where(first, other[0:1, :], mine[0:1, :])
    entropy = jnp.where(first, mine[1:2, :], other[1:2, :])
    live = extras[3:4, :]
    loss, weight, ent = token_terms(logp_c, logp_p, entropy, extras[1:2, :], extras[2:3, :], live)
    count = jnp.sum(live, axis=1, keepdims=True)
    lane = lax.broadcasted_iota(jnp.int32, (1, 3), 1)
    summary = jnp.where(lane == 0, jnp.sum(loss, axis=1, keepdims=True), 0.0)
    summary = jnp.where(lane == 1, jnp.sum(weight, axis=1, keepdims=True), summary)
    summary = jnp.where(lane == 2, jnp.sum(ent, axis=1, keepdims=True), summary)
    summary_out[...] = summary / count
    lines[0:1, :] = loss
    lines[1:2, :] = logp_c
    block = lines[:, pl.ds(pl.multiple_of(scal[1] * 128, 128), 128)]
    block = pltpu.roll(block, scal[4], 1)
    loss_out[...] = block[0:1, 0:8]
    logp_out[...] = block[1:2, 0:8]


def merge(a, b):
    peak = jnp.maximum(a[0:1], b[0:1])
    fa, fb = jnp.exp(a[0:1] - peak), jnp.exp(b[0:1] - peak)
    return jnp.concatenate([peak, a[1:3] * fa + b[1:3] * fb, a[3:4] + b[3:4]], axis=0)


def token_terms(logp_current, logp_proximal, entropy, advantages, behavior, live):
    ratio = jnp.exp(logp_current - logp_proximal)
    clipped = jnp.clip(ratio, 1.0 - CLIP_EPS, 1.0 + CLIP_EPS)
    surrogate = jnp.maximum(-advantages * ratio, -advantages * clipped)
    weight = jnp.minimum(jnp.exp(logp_proximal - behavior), WEIGHT_CAP)
    return (surrogate * weight * live, weight * live, entropy * live)


def either(first, a, b):
    return jnp.where(first, jnp.concatenate([a, b], axis=0), jnp.concatenate([b, a], axis=0))


def local(
    hidden_current,
    hidden_proximal,
    head_current,
    head_proximal,
    targets,
    loss_mask,
    lengths,
    behavior_logprob,
    advantages,
):
    f32, bf16 = jnp.float32, jnp.bfloat16
    own, depth = hidden_current.shape
    columns = head_current.shape[1]
    tokens = own * 128
    x, y, core, z = [lax.axis_index(a) for a in AXES]
    device = index_of(x, y, core, z)
    first = core == 0
    low = [(v & 1) ^ (v >> 1) for v in (x, y, z)]
    high = [v >> 1 for v in (x, y, z)]
    early_bits, late_bits = [], []
    for dim in range(3):
        pair = (low[dim], high[dim]) if LATE_BIT[0][dim] else (high[dim], low[dim])
        early_bits.append(jnp.where(first, pair[0], pair[1]))
        late_bits.append(jnp.where(first, pair[1], pair[0]))
    early_at = early_bits[0] + 2 * early_bits[1] + 4 * early_bits[2]
    late_at = late_bits[0] + 2 * late_bits[1] + 4 * late_bits[2]
    back = (128 - early_at * 16 - core * 8) % 128
    scal = jnp.stack([core, late_at, device * columns, (device ^ 4) * columns, back, early_bits[2]])
    scal = scal.astype(jnp.int32)

    lines = [targets, loss_mask, jnp.broadcast_to(lengths, (own,)), advantages, behavior_logprob]
    extra = pl.pallas_call(
        extra_kernel,
        out_shape=jax.ShapeDtypeStruct((own, EXTRA), bf16),
        in_specs=[VMEM],
        out_specs=VMEM,
        compiler_params=SMALL,
        name="extra",
    )(jnp.stack([v.astype(f32) for v in lines]))
    keep = jnp.concatenate([jnp.where(first, hidden_current, hidden_proximal), extra], axis=1)
    give = jnp.concatenate([jnp.where(first, hidden_proximal, hidden_current), extra], axis=1)
    block = either(first, keep, swap_core(give))
    heads_c, heads_p, block = lax.optimization_barrier((head_current.T, head_proximal.T, block))
    other_c = swap_core(heads_c)
    other_p = swap_core(heads_p)

    def load(for_c, for_p, limit):
        return pl.pallas_call(
            load_kernel,
            out_shape=jax.ShapeDtypeStruct((columns, depth), bf16),
            in_specs=[SMEM, HBM, HBM],
            out_specs=VMEM,
            scratch_shapes=[pltpu.SemaphoreType.DMA((1,))],
            compiler_params=pltpu.CompilerParams(vmem_limit_bytes=limit * 1024 * 1024),
            cost_estimate=pl.CostEstimate(
                flops=4 * 512 * 2048 * 256, bytes_accessed=4 * columns * depth, transcendentals=0
            ),
            name="load_head",
        )(scal, for_c, for_p)

    w0 = load(heads_c, heads_p, 46)
    got = swap(block, 0, 0)
    w0, got = lax.optimization_barrier((w0, got))
    block = either(early_bits[0] == 0, block, got)
    block = either(early_bits[1] == 0, block, swap(block, 1, 0))

    weights = [(0, 0, 1.0), (0, 1, 256.0), (0, 2, 65536.0)]
    weights += [(1, 3 + k, 1.0) for k in range(3)]
    weights += [(2, 6 + k, 1.0) for k in range(3)] + [(3, 9, 1.0)]
    table = np.zeros((8, EXTRA), np.float32)
    for a, b, w in weights:
        table[a, b] = w
    sel = jnp.asarray(table, bf16)

    cost = pl.CostEstimate(
        flops=4 * 256 * columns * depth,
        bytes_accessed=4 * columns * depth,
        transcendentals=2 * 256 * columns,
    )
    limit = pltpu.CompilerParams(vmem_limit_bytes=24 * 1024 * 1024)
    hidden = pltpu.VMEM((256, depth), bf16)

    def chunk(*pieces):
        return pl.pallas_call(
            chunk_kernel,
            out_shape=jax.ShapeDtypeStruct((8, 256), f32),
            in_specs=[SMEM] + [VMEM] * (3 + len(pieces)),
            out_specs=VMEM,
            scratch_shapes=[hidden],
            compiler_params=limit,
            cost_estimate=cost,
            name="chunk_stats",
        )(scal, w0, w1, sel, *pieces)

    half = block.shape[0]
    across = swap(block, 2, 0)
    one = [swap(block, dim, 1) for dim in range(3)]
    two = [swap(across, dim, 1) for dim in range(3)]
    other_c, other_p, across = lax.optimization_barrier((other_c, other_p, across))
    w1 = load(other_c, other_p, 31)
    near_one = chunk(block, *one)
    for dim in range(3):
        near_one, two[dim] = lax.optimization_barrier((near_one, two[dim]))
    both = [jnp.concatenate([one[dim], two[dim]], axis=0) for dim in range(3)]
    group = {3: swap(both[1], 0, 1), 6: swap(both[2], 1, 1), 5: swap(both[0], 2, 1)}
    near_two = chunk(across, *two)
    near_two, group[5], group[3] = lax.optimization_barrier((near_two, group[5], group[3]))
    part_one = swap(group[5][:half], 1, 1)
    part_two = swap(group[3][half:], 2, 1)
    third = chunk(group[3], group[5])
    stats, extras = pl.pallas_call(
        last_kernel,
        out_shape=(jax.ShapeDtypeStruct((4, tokens), f32),) * 2,
        in_specs=[SMEM] + [VMEM] * 9,
        out_specs=(VMEM, VMEM),
        scratch_shapes=[hidden, pltpu.VMEM((8, 256), f32)],
        compiler_params=limit,
        cost_estimate=cost,
        name="last_stats",
    )(scal, w0, w1, sel, near_one, near_two, third, group[6], part_one, part_two)

    for late in (0, 1):
        for dim in range(3):
            stats = merge(stats, swap(stats, dim, late))

    lse = stats[0:1] + jnp.log(stats[1:2])
    mine = jnp.concatenate([stats[3:4] - lse, lse - stats[2:3] / stats[1:2]], axis=0)
    other = swap_core(mine).reshape(2, 8, 8, 16).swapaxes(1, 2).reshape(2, tokens)
    loss, logp, summary = pl.pallas_call(
        final_kernel,
        out_shape=(
            jax.ShapeDtypeStruct((1, own), f32),
            jax.ShapeDtypeStruct((1, own), f32),
            jax.ShapeDtypeStruct((1, 3), f32),
        ),
        in_specs=[SMEM, VMEM, VMEM, VMEM],
        out_specs=(VMEM, VMEM, VMEM),
        scratch_shapes=[pltpu.VMEM((8, tokens), f32)],
        compiler_params=SMALL,
        name="final",
    )(scal, mine, other, extras)
    return (loss.reshape(own), logp.reshape(own), summary.reshape(3))


def solution(mesh):
    torus = Mesh(mesh.devices.reshape(4, 4, 2, mesh.shape["vocab"]), AXES)
    spec = P(AXES)
    return jax.shard_map(
        local,
        mesh=torus,
        in_specs=(P(AXES, None), P(AXES, None), P(None, AXES), P(None, AXES)) + (spec,) * 5,
        out_specs=(spec, spec, P()),
        check_vma=False,
    )
```

```python
import jax
import jax.numpy as jnp
import numpy as np
from jax import lax
from jax.experimental import pallas as pl
from jax.experimental.pallas import tpu as pltpu
from jax.sharding import Mesh
from jax.sharding import PartitionSpec as P

AXES = ("dp_0", "dp_1", "dp_2", "vocab")
SIZES = (4, 4, 2, 4)
CLIP_EPS = 0.2
WEIGHT_CAP = 5.0
EXTRA = 128
LATE_BIT = ((1, 0, 0), (0, 1, 1))


def flip(coordinate, bit):
    return coordinate ^ 1 if bit == 0 else 3 - coordinate


def index_of(x, y, c, z):
    return ((x * 4 + y) * 2 + c) * 4 + z


def swap_pairs(dim, late):
    pairs = []
    for x in range(4):
        for y in range(4):
            for c in range(2):
                for z in range(4):
                    bit = LATE_BIT[c][dim] if late else 1 - LATE_BIT[c][dim]
                    to = [x, y, z]
                    to[dim] = flip(to[dim], bit)
                    pairs.append((index_of(x, y, c, z), index_of(to[0], to[1], c, to[2])))
    return pairs


def swap(value, dim, late):
    return lax.ppermute(value, AXES, swap_pairs(dim, late))


def swap_core(value):
    return lax.ppermute(value, AXES, [(k, k ^ 4) for k in range(128)])


VMEM = pl.BlockSpec(memory_space=pltpu.VMEM)
SMEM = pl.BlockSpec(memory_space=pltpu.SMEM)
HBM = pl.BlockSpec(memory_space=pltpu.HBM)
NT = (((1,), (1,)), ((), ()))
SMALL = pltpu.CompilerParams(vmem_limit_bytes=4 * 1024 * 1024)


def column_of(line):
    rows = lax.broadcasted_iota(jnp.int32, (8, 8), 0)
    lanes = lax.broadcasted_iota(jnp.int32, (8, 8), 1)
    spread = jnp.broadcast_to(line, (8, 8))
    return jnp.sum(jnp.where(rows == lanes, spread, 0.0), axis=1, keepdims=True)


def three_parts(value):
    high = value.astype(jnp.bfloat16).astype(jnp.float32)
    middle = (value - high).astype(jnp.bfloat16).astype(jnp.float32)
    return [high, middle, value - high - middle]


def extra_kernel(lines, extra):
    ids = lines[0:1, :].astype(jnp.int32)
    place = lax.broadcasted_iota(jnp.int32, (1, 8), 1).astype(jnp.float32)
    live = jnp.where((place < lines[2:3, :]) & (lines[1:2, :] == 1.0), 1.0, 0.0)
    values = [v.astype(jnp.float32) for v in (ids & 255, (ids >> 8) & 255, ids >> 16)]
    values += three_parts(lines[3:4, :]) + three_parts(lines[4:5, :]) + [live]
    lane = lax.broadcasted_iota(jnp.int32, extra.shape, 1)
    table = jnp.zeros(extra.shape, jnp.float32)
    for k, value in enumerate(values):
        table = jnp.where(lane == k, column_of(value), table)
    extra[...] = table.astype(jnp.bfloat16)


def load_kernel(scal, for_c, for_p, weights, sem):
    for core, source in enumerate((for_c, for_p)):

        @pl.when(scal[0] == core)
        def _(source=source):
            pltpu.make_async_copy(source, weights, sem.at[0]).start()

    pltpu.make_async_copy(for_c, weights, sem.at[0]).wait()


def chunk_stats(scal, w0, w1, sel, pieces, hidden, out):
    depth = hidden.shape[1]
    at = 0
    for piece in pieces:
        rows = piece.shape[0]
        hidden[at : at + rows, :] = piece[:, :depth]
        out[4:8, at : at + rows] = lax.dot_general(
            sel[...], piece[:, depth:], NT, preferred_element_type=jnp.float32
        )[0:4]
        at += rows
    target = out[4:5, :].astype(jnp.int32)
    before = None
    for h, weights in enumerate((w0, w1)):
        logits = lax.dot_general(
            weights[...], hidden[...], NT, preferred_element_type=jnp.float32
        )
        wanted = target - scal[2 + h]
        peak = jnp.max(logits, axis=0, keepdims=True)
        if before is not None:
            peak = jnp.maximum(peak, before[0])
        powers = jnp.exp(logits - peak)
        total = jnp.sum(powers, axis=0, keepdims=True)
        moment = jnp.sum(powers * logits, axis=0, keepdims=True)
        row = lax.broadcasted_iota(jnp.int32, logits.shape, 0)
        picked = jnp.sum(jnp.where(row == wanted, logits, 0.0), axis=0, keepdims=True)
        if before is not None:
            scale = jnp.exp(before[0] - peak)
            total = total + before[1] * scale
            moment = moment + before[2] * scale
            picked = picked + before[3]
        before = (peak, total, moment, picked)
    for k in range(4):
        out[k : k + 1, :] = before[k]


def chunk_kernel(scal, w0, w1, sel, *refs):
    chunk_stats(scal, w0, w1, sel, refs[:-2], refs[-1], refs[-2])


def last_kernel(scal, w0, w1, sel, *refs):
    (near_one, near_two, third), pieces = refs[:3], refs[3:-4]
    stats, extras, hidden, mine = refs[-4:]
    chunk_stats(scal, w0, w1, sel, pieces, hidden, mine)
    left = lax.broadcasted_iota(jnp.int32, (8, 128), 1) < 64
    blocks = {}
    one, two = near_one[:, 128:], near_two[:, :128]
    blocks[0] = near_one[:, :128]
    blocks[1] = jnp.where(left, one, pltpu.roll(two, 64, 1))
    blocks[2] = jnp.where(left, pltpu.roll(one, 64, 1), two)
    blocks[4] = near_two[:, 128:]
    for chunk, pair in ((third, (3, 5)), (mine, (6, 7))):
        for k in range(2):
            blocks[pair[k]] = chunk[:, k * 128 : (k + 1) * 128]
    for relative, block in blocks.items():
        block = jnp.where(scal[5] == 1, pltpu.roll(block, 64, 1), block)
        lanes = pl.ds(pl.multiple_of((relative ^ scal[1]) * 128, 128), 128)
        stats[:, lanes] = block[0:4]
        extras[:, lanes] = block[4:8]


def final_kernel(scal, mine, other, extras, loss_out, logp_out, summary_out, lines):
    first = scal[0] == 0
    logp_c = jnp.where(first, mine[0:1, :], other[0:1, :])
    logp_p = jnp.where(first, other[0:1, :], mine[0:1, :])
    entropy = jnp.where(first, mine[1:2, :], other[1:2, :])
    live = extras[3:4, :]
    loss, weight, ent = token_terms(logp_c, logp_p, entropy, extras[1:2, :], extras[2:3, :], live)
    count = jnp.sum(live, axis=1, keepdims=True)
    lane = lax.broadcasted_iota(jnp.int32, (1, 3), 1)
    summary = jnp.where(lane == 0, jnp.sum(loss, axis=1, keepdims=True), 0.0)
    summary = jnp.where(lane == 1, jnp.sum(weight, axis=1, keepdims=True), summary)
    summary = jnp.where(lane == 2, jnp.sum(ent, axis=1, keepdims=True), summary)
    summary_out[...] = summary / count
    lines[0:1, :] = loss
    lines[1:2, :] = logp_c
    block = lines[:, pl.ds(pl.multiple_of(scal[1] * 128, 128), 128)]
    block = pltpu.roll(block, scal[4], 1)
    loss_out[...] = block[0:1, 0:8]
    logp_out[...] = block[1:2, 0:8]


def merge(a, b):
    peak = jnp.maximum(a[0:1], b[0:1])
    fa, fb = jnp.exp(a[0:1] - peak), jnp.exp(b[0:1] - peak)
    return jnp.concatenate([peak, a[1:3] * fa + b[1:3] * fb, a[3:4] + b[3:4]], axis=0)


def token_terms(logp_current, logp_proximal, entropy, advantages, behavior, live):
    ratio = jnp.exp(logp_current - logp_proximal)
    clipped = jnp.clip(ratio, 1.0 - CLIP_EPS, 1.0 + CLIP_EPS)
    surrogate = jnp.maximum(-advantages * ratio, -advantages * clipped)
    weight = jnp.minimum(jnp.exp(logp_proximal - behavior), WEIGHT_CAP)
    return (surrogate * weight * live, weight * live, entropy * live)


def either(first, a, b):
    return jnp.where(first, jnp.concatenate([a, b], axis=0), jnp.concatenate([b, a], axis=0))


def local(
    hidden_current,
    hidden_proximal,
    head_current,
    head_proximal,
    targets,
    loss_mask,
    lengths,
    behavior_logprob,
    advantages,
):
    f32, bf16 = jnp.float32, jnp.bfloat16
    own, depth = hidden_current.shape
    columns = head_current.shape[1]
    tokens = own * 128
    x, y, core, z = [lax.axis_index(a) for a in AXES]
    device = index_of(x, y, core, z)
    first = core == 0
    low = [(v & 1) ^ (v >> 1) for v in (x, y, z)]
    high = [v >> 1 for v in (x, y, z)]
    early_bits, late_bits = [], []
    for dim in range(3):
        pair = (low[dim], high[dim]) if LATE_BIT[0][dim] else (high[dim], low[dim])
        early_bits.append(jnp.where(first, pair[0], pair[1]))
        late_bits.append(jnp.where(first, pair[1], pair[0]))
    early_at = early_bits[0] + 2 * early_bits[1] + 4 * early_bits[2]
    late_at = late_bits[0] + 2 * late_bits[1] + 4 * late_bits[2]
    back = (128 - early_at * 16 - core * 8) % 128
    scal = jnp.stack([core, late_at, device * columns, (device ^ 4) * columns, back, early_bits[2]])
    scal = scal.astype(jnp.int32)

    lines = [targets, loss_mask, jnp.broadcast_to(lengths, (own,)), advantages, behavior_logprob]
    extra = pl.pallas_call(
        extra_kernel,
        out_shape=jax.ShapeDtypeStruct((own, EXTRA), bf16),
        in_specs=[VMEM],
        out_specs=VMEM,
        compiler_params=SMALL,
        name="extra",
    )(jnp.stack([v.astype(f32) for v in lines]))
    keep = jnp.concatenate([jnp.where(first, hidden_current, hidden_proximal), extra], axis=1)
    give = jnp.concatenate([jnp.where(first, hidden_proximal, hidden_current), extra], axis=1)
    block = either(first, keep, swap_core(give))
    heads_c, heads_p, block = lax.optimization_barrier((head_current.T, head_proximal.T, block))
    other_c = swap_core(heads_c)
    other_p = swap_core(heads_p)

    def load(for_c, for_p, limit):
        return pl.pallas_call(
            load_kernel,
            out_shape=jax.ShapeDtypeStruct((columns, depth), bf16),
            in_specs=[SMEM, HBM, HBM],
            out_specs=VMEM,
            scratch_shapes=[pltpu.SemaphoreType.DMA((1,))],
            compiler_params=pltpu.CompilerParams(vmem_limit_bytes=limit * 1024 * 1024),
            cost_estimate=pl.CostEstimate(
                flops=4 * 512 * 2048 * 256, bytes_accessed=4 * columns * depth, transcendentals=0
            ),
            name="load_head",
        )(scal, for_c, for_p)

    block = either(early_bits[0] == 0, block, swap(block, 0, 0))
    heads_c, heads_p, block = lax.optimization_barrier((heads_c, heads_p, block))
    w0 = load(heads_c, heads_p, 46)
    got = swap(block, 1, 0)
    w0, got = lax.optimization_barrier((w0, got))
    block = either(early_bits[1] == 0, block, got)

    weights = [(0, 0, 1.0), (0, 1, 256.0), (0, 2, 65536.0)]
    weights += [(1, 3 + k, 1.0) for k in range(3)]
    weights += [(2, 6 + k, 1.0) for k in range(3)] + [(3, 9, 1.0)]
    table = np.zeros((8, EXTRA), np.float32)
    for a, b, w in weights:
        table[a, b] = w
    sel = jnp.asarray(table, bf16)

    cost = pl.CostEstimate(
        flops=4 * 256 * columns * depth,
        bytes_accessed=4 * columns * depth,
        transcendentals=2 * 256 * columns,
    )
    limit = pltpu.CompilerParams(vmem_limit_bytes=24 * 1024 * 1024)
    hidden = pltpu.VMEM((256, depth), bf16)

    def chunk(*pieces):
        return pl.pallas_call(
            chunk_kernel,
            out_shape=jax.ShapeDtypeStruct((8, 256), f32),
            in_specs=[SMEM] + [VMEM] * (3 + len(pieces)),
            out_specs=VMEM,
            scratch_shapes=[hidden],
            compiler_params=limit,
            cost_estimate=cost,
            name="chunk_stats",
        )(scal, w0, w1, sel, *pieces)

    half = block.shape[0]
    across = swap(block, 2, 0)
    one = [swap(block, dim, 1) for dim in range(2)]
    two = [swap(across, dim, 1) for dim in range(2)]
    group = {4: swap(jnp.concatenate([block, across], axis=0), 2, 1)}
    other_c, other_p, across = lax.optimization_barrier((other_c, other_p, across))
    w1 = load(other_c, other_p, 31)
    w1, two[0], two[1] = lax.optimization_barrier((w1, two[0], two[1]))
    both = [jnp.concatenate([one[dim], two[dim]], axis=0) for dim in range(2)]
    near_one = chunk(block, across, *one)
    near_one, group[4] = lax.optimization_barrier((near_one, group[4]))
    group |= {3: swap(both[1], 0, 1), 5: swap(both[0], 2, 1), 6: swap(group[4], 1, 1)}
    near_two = chunk(*two, group[4])
    near_one, near_two, group[5], group[3] = lax.optimization_barrier(
        (near_one, near_two, group[5], group[3])
    )
    part_one = swap(group[5][:half], 1, 1)
    part_two = swap(group[3][half:], 2, 1)
    third = chunk(group[3], group[5])
    stats, extras = pl.pallas_call(
        last_kernel,
        out_shape=(jax.ShapeDtypeStruct((4, tokens), f32),) * 2,
        in_specs=[SMEM] + [VMEM] * 9,
        out_specs=(VMEM, VMEM),
        scratch_shapes=[hidden, pltpu.VMEM((8, 256), f32)],
        compiler_params=limit,
        cost_estimate=cost,
        name="last_stats",
    )(scal, w0, w1, sel, near_one, near_two, third, group[6], part_one, part_two)

    for late in (0, 1):
        for dim in range(3):
            stats = merge(stats, swap(stats, dim, late))

    lse = stats[0:1] + jnp.log(stats[1:2])
    mine = jnp.concatenate([stats[3:4] - lse, lse - stats[2:3] / stats[1:2]], axis=0)
    other = swap_core(mine).reshape(2, 8, 8, 16).swapaxes(1, 2).reshape(2, tokens)
    loss, logp, summary = pl.pallas_call(
        final_kernel,
        out_shape=(
            jax.ShapeDtypeStruct((1, own), f32),
            jax.ShapeDtypeStruct((1, own), f32),
            jax.ShapeDtypeStruct((1, 3), f32),
        ),
        in_specs=[SMEM, VMEM, VMEM, VMEM],
        out_specs=(VMEM, VMEM, VMEM),
        scratch_shapes=[pltpu.VMEM((8, tokens), f32)],
        compiler_params=SMALL,
        name="final",
    )(scal, mine, other, extras)
    return (loss.reshape(own), logp.reshape(own), summary.reshape(3))


def solution(mesh):
    torus = Mesh(mesh.devices.reshape(4, 4, 2, mesh.shape["vocab"]), AXES)
    spec = P(AXES)
    return jax.shard_map(
        local,
        mesh=torus,
        in_specs=(P(AXES, None), P(AXES, None), P(None, AXES), P(None, AXES)) + (spec,) * 5,
        out_specs=(spec, spec, P()),
        check_vma=False,
    )
```

```python
import functools

import jax
import jax.numpy as jnp
import numpy as np
from jax import lax
from jax.experimental import pallas as pl
from jax.experimental.pallas import tpu as pltpu
from jax.sharding import Mesh
from jax.sharding import PartitionSpec as P

AXES = ("dp_0", "dp_1", "dp_2", "vocab")
SIZES = (4, 4, 2, 4)
CLIP_EPS = 0.2
WEIGHT_CAP = 5.0
EXTRA = 128
LATE_BIT = ((1, 0, 0), (0, 1, 1))


def flip(coordinate, bit):
    return coordinate ^ 1 if bit == 0 else 3 - coordinate


def index_of(x, y, c, z):
    return ((x * 4 + y) * 2 + c) * 4 + z


def swap_pairs(dims, late):
    pairs = []
    for x in range(4):
        for y in range(4):
            for c in range(2):
                for z in range(4):
                    to = [x, y, z]
                    for dim in dims:
                        bit = LATE_BIT[c][dim] if late else 1 - LATE_BIT[c][dim]
                        to[dim] = flip(to[dim], bit)
                    pairs.append((index_of(x, y, c, z), index_of(to[0], to[1], c, to[2])))
    return pairs


def swap(value, dims, late):
    dims = (dims,) if isinstance(dims, int) else dims
    return lax.ppermute(value, AXES, swap_pairs(dims, late))


def shift(value, dim, by):
    pairs = []
    for x in range(4):
        for y in range(4):
            for c in range(2):
                for z in range(4):
                    to = [x, y, z]
                    to[dim] = (to[dim] + by) % 4
                    pairs.append((index_of(x, y, c, z), index_of(to[0], to[1], c, to[2])))
    return lax.ppermute(value, AXES, pairs)


def swap_core(value):
    return lax.ppermute(value, AXES, [(k, k ^ 4) for k in range(128)])


VMEM = pl.BlockSpec(memory_space=pltpu.VMEM)
SMEM = pl.BlockSpec(memory_space=pltpu.SMEM)
HBM = pl.BlockSpec(memory_space=pltpu.HBM)
NT = (((1,), (1,)), ((), ()))
SMALL = pltpu.CompilerParams(vmem_limit_bytes=4 * 1024 * 1024)


def column_of(line):
    rows = lax.broadcasted_iota(jnp.int32, (8, 8), 0)
    lanes = lax.broadcasted_iota(jnp.int32, (8, 8), 1)
    spread = jnp.broadcast_to(line, (8, 8))
    return jnp.sum(jnp.where(rows == lanes, spread, 0.0), axis=1, keepdims=True)


def three_parts(value):
    high = value.astype(jnp.bfloat16).astype(jnp.float32)
    middle = (value - high).astype(jnp.bfloat16).astype(jnp.float32)
    return [high, middle, value - high - middle]


def extra_kernel(lines, extra):
    ids = lines[0:1, :].astype(jnp.int32)
    place = lax.broadcasted_iota(jnp.int32, (1, 8), 1).astype(jnp.float32)
    live = jnp.where((place < lines[2:3, :]) & (lines[1:2, :] == 1.0), 1.0, 0.0)
    values = [v.astype(jnp.float32) for v in (ids & 255, (ids >> 8) & 255, ids >> 16)]
    values += three_parts(lines[3:4, :]) + three_parts(lines[4:5, :]) + [live]
    lane = lax.broadcasted_iota(jnp.int32, extra.shape, 1)
    table = jnp.zeros(extra.shape, jnp.float32)
    for k, value in enumerate(values):
        table = jnp.where(lane == k, column_of(value), table)
    extra[...] = table.astype(jnp.bfloat16)


def load_kernel(scal, for_c, for_p, weights, sem):
    for core, source in enumerate((for_c, for_p)):

        @pl.when(scal[0] == core)
        def _(source=source):
            pltpu.make_async_copy(source, weights, sem.at[0]).start()

    pltpu.make_async_copy(for_c, weights, sem.at[0]).wait()


def chunk_stats(scal, w0, w1, sel, pieces, hidden, out):
    depth = hidden.shape[1]
    at = 0
    for piece in pieces:
        rows = piece.shape[0]
        hidden[at : at + rows, :] = piece[:, :depth]
        out[4:8, at : at + rows] = lax.dot_general(
            sel[...], piece[:, depth:], NT, preferred_element_type=jnp.float32
        )[0:4]
        at += rows
    target = out[4:5, :].astype(jnp.int32)
    before = None
    for h, weights in enumerate((w0, w1)):
        logits = lax.dot_general(
            weights[...], hidden[...], NT, preferred_element_type=jnp.float32
        )
        wanted = target - scal[2 + h]
        peak = jnp.max(logits, axis=0, keepdims=True)
        if before is not None:
            peak = jnp.maximum(peak, before[0])
        powers = jnp.exp(logits - peak)
        total = jnp.sum(powers, axis=0, keepdims=True)
        moment = jnp.sum(powers * logits, axis=0, keepdims=True)
        row = lax.broadcasted_iota(jnp.int32, logits.shape, 0)
        picked = jnp.sum(jnp.where(row == wanted, logits, 0.0), axis=0, keepdims=True)
        if before is not None:
            scale = jnp.exp(before[0] - peak)
            total = total + before[1] * scale
            moment = moment + before[2] * scale
            picked = picked + before[3]
        before = (peak, total, moment, picked)
    for k in range(4):
        out[k : k + 1, :] = before[k]


def chunk_kernel(scal, w0, w1, sel, *refs):
    chunk_stats(scal, w0, w1, sel, refs[:-2], refs[-1], refs[-2])


def last_kernel(scal, w0, w1, sel, *refs):
    (near_one, near_two, third), pieces = refs[:3], refs[3:-4]
    stats, extras, hidden, mine = refs[-4:]
    chunk_stats(scal, w0, w1, sel, pieces, hidden, mine)
    left = lax.broadcasted_iota(jnp.int32, (8, 128), 1) < 64
    blocks = {}
    one, two = near_one[:, 128:], near_two[:, :128]
    blocks[0] = near_one[:, :128]
    blocks[1] = jnp.where(left, one, pltpu.roll(two, 64, 1))
    blocks[2] = jnp.where(left, pltpu.roll(one, 64, 1), two)
    blocks[4] = near_two[:, 128:]
    for chunk, pair in ((third, (3, 5)), (mine, (6, 7))):
        for k in range(2):
            blocks[pair[k]] = chunk[:, k * 128 : (k + 1) * 128]
    for relative, block in blocks.items():
        block = jnp.where(scal[5] == 1, pltpu.roll(block, 64, 1), block)
        lanes = pl.ds(pl.multiple_of((relative ^ scal[1]) * 128, 128), 128)
        stats[:, lanes] = block[0:4]
        extras[:, lanes] = block[4:8]


def final_kernel(scal, mine, other, extras, loss_out, logp_out, summary_out, lines):
    first = scal[0] == 0
    logp_c = jnp.where(first, mine[0:1, :], other[0:1, :])
    logp_p = jnp.where(first, other[0:1, :], mine[0:1, :])
    entropy = jnp.where(first, mine[1:2, :], other[1:2, :])
    live = extras[3:4, :]
    loss, weight, ent = token_terms(logp_c, logp_p, entropy, extras[1:2, :], extras[2:3, :], live)
    count = jnp.sum(live, axis=1, keepdims=True)
    lane = lax.broadcasted_iota(jnp.int32, (1, 3), 1)
    summary = jnp.where(lane == 0, jnp.sum(loss, axis=1, keepdims=True), 0.0)
    summary = jnp.where(lane == 1, jnp.sum(weight, axis=1, keepdims=True), summary)
    summary = jnp.where(lane == 2, jnp.sum(ent, axis=1, keepdims=True), summary)
    summary_out[...] = summary / count
    lines[0:1, :] = loss
    lines[1:2, :] = logp_c
    block = lines[:, pl.ds(pl.multiple_of(scal[1] * 128, 128), 128)]
    block = pltpu.roll(block, scal[4], 1)
    loss_out[...] = block[0:1, 0:8]
    logp_out[...] = block[1:2, 0:8]


def merge(a, b):
    peak = jnp.maximum(a[0:1], b[0:1])
    fa, fb = jnp.exp(a[0:1] - peak), jnp.exp(b[0:1] - peak)
    return jnp.concatenate([peak, a[1:3] * fa + b[1:3] * fb, a[3:4] + b[3:4]], axis=0)


def merge_ring(own, others):
    every = [own, *others]
    peak = functools.reduce(jnp.maximum, [v[0:1] for v in every])
    scales = [jnp.exp(v[0:1] - peak) for v in every]
    sums = sum(v[1:3] * f for v, f in zip(every, scales))
    return jnp.concatenate([peak, sums, sum(v[3:4] for v in every)], axis=0)


def token_terms(logp_current, logp_proximal, entropy, advantages, behavior, live):
    ratio = jnp.exp(logp_current - logp_proximal)
    clipped = jnp.clip(ratio, 1.0 - CLIP_EPS, 1.0 + CLIP_EPS)
    surrogate = jnp.maximum(-advantages * ratio, -advantages * clipped)
    weight = jnp.minimum(jnp.exp(logp_proximal - behavior), WEIGHT_CAP)
    return (surrogate * weight * live, weight * live, entropy * live)


def either(first, a, b):
    return jnp.where(first, jnp.concatenate([a, b], axis=0), jnp.concatenate([b, a], axis=0))


def local(
    hidden_current,
    hidden_proximal,
    head_current,
    head_proximal,
    targets,
    loss_mask,
    lengths,
    behavior_logprob,
    advantages,
):
    f32, bf16 = jnp.float32, jnp.bfloat16
    own, depth = hidden_current.shape
    columns = head_current.shape[1]
    tokens = own * 128
    x, y, core, z = [lax.axis_index(a) for a in AXES]
    device = index_of(x, y, core, z)
    first = core == 0
    low = [(v & 1) ^ (v >> 1) for v in (x, y, z)]
    high = [v >> 1 for v in (x, y, z)]
    early_bits, late_bits = [], []
    for dim in range(3):
        pair = (low[dim], high[dim]) if LATE_BIT[0][dim] else (high[dim], low[dim])
        early_bits.append(jnp.where(first, pair[0], pair[1]))
        late_bits.append(jnp.where(first, pair[1], pair[0]))
    early_at = early_bits[0] + 2 * early_bits[1] + 4 * early_bits[2]
    late_at = late_bits[0] + 2 * late_bits[1] + 4 * late_bits[2]
    back = (128 - early_at * 16 - core * 8) % 128
    scal = jnp.stack([core, late_at, device * columns, (device ^ 4) * columns, back, early_bits[2]])
    scal = scal.astype(jnp.int32)

    lines = [targets, loss_mask, jnp.broadcast_to(lengths, (own,)), advantages, behavior_logprob]
    extra = pl.pallas_call(
        extra_kernel,
        out_shape=jax.ShapeDtypeStruct((own, EXTRA), bf16),
        in_specs=[VMEM],
        out_specs=VMEM,
        compiler_params=SMALL,
        name="extra",
    )(jnp.stack([v.astype(f32) for v in lines]))
    keep = jnp.concatenate([jnp.where(first, hidden_current, hidden_proximal), extra], axis=1)
    give = jnp.concatenate([jnp.where(first, hidden_proximal, hidden_current), extra], axis=1)
    block = either(first, keep, swap_core(give))
    heads_c, heads_p, block = lax.optimization_barrier((head_current.T, head_proximal.T, block))
    other_c = swap_core(heads_c)
    other_p = swap_core(heads_p)

    def load(for_c, for_p, limit):
        return pl.pallas_call(
            load_kernel,
            out_shape=jax.ShapeDtypeStruct((columns, depth), bf16),
            in_specs=[SMEM, HBM, HBM],
            out_specs=VMEM,
            scratch_shapes=[pltpu.SemaphoreType.DMA((1,))],
            compiler_params=pltpu.CompilerParams(vmem_limit_bytes=limit * 1024 * 1024),
            cost_estimate=pl.CostEstimate(
                flops=4 * 512 * 2048 * 256, bytes_accessed=4 * columns * depth, transcendentals=0
            ),
            name="load_head",
        )(scal, for_c, for_p)

    w0 = load(heads_c, heads_p, 46)
    got = [swap(block, dims, 0) for dims in (0, 1, (0, 1))]
    w0, *got = lax.optimization_barrier((w0, *got))
    across_x = [either(early_bits[0] == 0, a, b) for a, b in ((block, got[0]), (got[1], got[2]))]
    block = either(early_bits[1] == 0, *across_x)

    weights = [(0, 0, 1.0), (0, 1, 256.0), (0, 2, 65536.0)]
    weights += [(1, 3 + k, 1.0) for k in range(3)]
    weights += [(2, 6 + k, 1.0) for k in range(3)] + [(3, 9, 1.0)]
    table = np.zeros((8, EXTRA), np.float32)
    for a, b, w in weights:
        table[a, b] = w
    sel = jnp.asarray(table, bf16)

    cost = pl.CostEstimate(
        flops=4 * 256 * columns * depth,
        bytes_accessed=4 * columns * depth,
        transcendentals=2 * 256 * columns,
    )
    limit = pltpu.CompilerParams(vmem_limit_bytes=24 * 1024 * 1024)
    hidden = pltpu.VMEM((256, depth), bf16)

    def chunk(*pieces):
        return pl.pallas_call(
            chunk_kernel,
            out_shape=jax.ShapeDtypeStruct((8, 256), f32),
            in_specs=[SMEM] + [VMEM] * (3 + len(pieces)),
            out_specs=VMEM,
            scratch_shapes=[hidden],
            compiler_params=limit,
            cost_estimate=cost,
            name="chunk_stats",
        )(scal, w0, w1, sel, *pieces)

    half = block.shape[0]
    across = swap(block, 2, 0)
    one = [swap(block, dim, 1) for dim in range(2)]
    two = [swap(across, dim, 1) for dim in range(2)]
    group = {4: swap(jnp.concatenate([block, across], axis=0), 2, 1)}
    other_c, other_p, across = lax.optimization_barrier((other_c, other_p, across))
    w1 = load(other_c, other_p, 31)
    w1, two[0], two[1] = lax.optimization_barrier((w1, two[0], two[1]))
    both = [jnp.concatenate([one[dim], two[dim]], axis=0) for dim in range(2)]
    near_one = chunk(block, across, *one)
    near_one, group[4] = lax.optimization_barrier((near_one, group[4]))
    group |= {3: swap(both[1], 0, 1), 5: swap(both[0], 2, 1), 6: swap(group[4], 1, 1)}
    near_two = chunk(*two, group[4])
    near_one, near_two, group[5], group[3] = lax.optimization_barrier(
        (near_one, near_two, group[5], group[3])
    )
    part_one = swap(group[5][:half], 1, 1)
    part_two = swap(group[3][half:], 2, 1)
    third = chunk(group[3], group[5])
    stats, extras = pl.pallas_call(
        last_kernel,
        out_shape=(jax.ShapeDtypeStruct((4, tokens), f32),) * 2,
        in_specs=[SMEM] + [VMEM] * 9,
        out_specs=(VMEM, VMEM),
        scratch_shapes=[hidden, pltpu.VMEM((8, 256), f32)],
        compiler_params=limit,
        cost_estimate=cost,
        name="last_stats",
    )(scal, w0, w1, sel, near_one, near_two, third, group[6], part_one, part_two)

    for dim in range(3):
        stats = merge_ring(stats, [shift(stats, dim, k) for k in (1, 3, 2)])

    lse = stats[0:1] + jnp.log(stats[1:2])
    mine = jnp.concatenate([stats[3:4] - lse, lse - stats[2:3] / stats[1:2]], axis=0)
    other = swap_core(mine).reshape(2, 8, 8, 16).swapaxes(1, 2).reshape(2, tokens)
    loss, logp, summary = pl.pallas_call(
        final_kernel,
        out_shape=(
            jax.ShapeDtypeStruct((1, own), f32),
            jax.ShapeDtypeStruct((1, own), f32),
            jax.ShapeDtypeStruct((1, 3), f32),
        ),
        in_specs=[SMEM, VMEM, VMEM, VMEM],
        out_specs=(VMEM, VMEM, VMEM),
        scratch_shapes=[pltpu.VMEM((8, tokens), f32)],
        compiler_params=SMALL,
        name="final",
    )(scal, mine, other, extras)
    return (loss.reshape(own), logp.reshape(own), summary.reshape(3))


def solution(mesh):
    torus = Mesh(mesh.devices.reshape(4, 4, 2, mesh.shape["vocab"]), AXES)
    spec = P(AXES)
    return jax.shard_map(
        local,
        mesh=torus,
        in_specs=(P(AXES, None), P(AXES, None), P(None, AXES), P(None, AXES)) + (spec,) * 5,
        out_specs=(spec, spec, P()),
        check_vma=False,
    )
```

```python
import functools

import jax
import jax.numpy as jnp
import numpy as np
from jax import lax
from jax.experimental import pallas as pl
from jax.experimental.pallas import tpu as pltpu
from jax.sharding import Mesh
from jax.sharding import PartitionSpec as P

AXES = ("dp_0", "dp_1", "dp_2", "vocab")
SIZES = (4, 4, 2, 4)
CLIP_EPS = 0.2
WEIGHT_CAP = 5.0
EXTRA = 128
LATE_BIT = ((1, 0, 0), (0, 1, 1))


def flip(coordinate, bit):
    return coordinate ^ 1 if bit == 0 else 3 - coordinate


def index_of(x, y, c, z):
    return ((x * 4 + y) * 2 + c) * 4 + z


def swap_pairs(dims, late):
    pairs = []
    for x in range(4):
        for y in range(4):
            for c in range(2):
                for z in range(4):
                    to = [x, y, z]
                    for dim in dims:
                        bit = LATE_BIT[c][dim] if late else 1 - LATE_BIT[c][dim]
                        to[dim] = flip(to[dim], bit)
                    pairs.append((index_of(x, y, c, z), index_of(to[0], to[1], c, to[2])))
    return pairs


def swap(value, dims, late):
    dims = (dims,) if isinstance(dims, int) else dims
    return lax.ppermute(value, AXES, swap_pairs(dims, late))


def shift(value, dim, by):
    pairs = []
    for x in range(4):
        for y in range(4):
            for c in range(2):
                for z in range(4):
                    to = [x, y, z]
                    to[dim] = (to[dim] + by) % 4
                    pairs.append((index_of(x, y, c, z), index_of(to[0], to[1], c, to[2])))
    return lax.ppermute(value, AXES, pairs)


def swap_core(value):
    return lax.ppermute(value, AXES, [(k, k ^ 4) for k in range(128)])


VMEM = pl.BlockSpec(memory_space=pltpu.VMEM)
SMEM = pl.BlockSpec(memory_space=pltpu.SMEM)
HBM = pl.BlockSpec(memory_space=pltpu.HBM)
NT = (((1,), (1,)), ((), ()))
SMALL = pltpu.CompilerParams(vmem_limit_bytes=4 * 1024 * 1024)


def column_of(line):
    rows = lax.broadcasted_iota(jnp.int32, (8, 8), 0)
    lanes = lax.broadcasted_iota(jnp.int32, (8, 8), 1)
    spread = jnp.broadcast_to(line, (8, 8))
    return jnp.sum(jnp.where(rows == lanes, spread, 0.0), axis=1, keepdims=True)


def three_parts(value):
    high = value.astype(jnp.bfloat16).astype(jnp.float32)
    middle = (value - high).astype(jnp.bfloat16).astype(jnp.float32)
    return [high, middle, value - high - middle]


def extra_kernel(lines, extra):
    ids = lines[0:1, :].astype(jnp.int32)
    place = lax.broadcasted_iota(jnp.int32, (1, 8), 1).astype(jnp.float32)
    live = jnp.where((place < lines[2:3, :]) & (lines[1:2, :] == 1.0), 1.0, 0.0)
    values = [v.astype(jnp.float32) for v in (ids & 255, (ids >> 8) & 255, ids >> 16)]
    values += three_parts(lines[3:4, :]) + three_parts(lines[4:5, :]) + [live]
    lane = lax.broadcasted_iota(jnp.int32, extra.shape, 1)
    table = jnp.zeros(extra.shape, jnp.float32)
    for k, value in enumerate(values):
        table = jnp.where(lane == k, column_of(value), table)
    extra[...] = table.astype(jnp.bfloat16)


def load_kernel(scal, for_c, for_p, weights, sem):
    for core, source in enumerate((for_c, for_p)):

        @pl.when(scal[0] == core)
        def _(source=source):
            pltpu.make_async_copy(source, weights, sem.at[0]).start()

    pltpu.make_async_copy(for_c, weights, sem.at[0]).wait()


def chunk_stats(scal, w0, w1, sel, pieces, hidden, out):
    depth = hidden.shape[1]
    at = 0
    for piece in pieces:
        rows = piece.shape[0]
        hidden[at : at + rows, :] = piece[:, :depth]
        out[4:8, at : at + rows] = lax.dot_general(
            sel[...], piece[:, depth:], NT, preferred_element_type=jnp.float32
        )[0:4]
        at += rows
    target = out[4:5, :].astype(jnp.int32)
    before = None
    for h, weights in enumerate((w0, w1)):
        logits = lax.dot_general(
            weights[...], hidden[...], NT, preferred_element_type=jnp.float32
        )
        wanted = target - scal[2 + h]
        peak = jnp.max(logits, axis=0, keepdims=True)
        if before is not None:
            peak = jnp.maximum(peak, before[0])
        powers = jnp.exp(logits - peak)
        total = jnp.sum(powers, axis=0, keepdims=True)
        moment = jnp.sum(powers * logits, axis=0, keepdims=True)
        row = lax.broadcasted_iota(jnp.int32, logits.shape, 0)
        picked = jnp.sum(jnp.where(row == wanted, logits, 0.0), axis=0, keepdims=True)
        if before is not None:
            scale = jnp.exp(before[0] - peak)
            total = total + before[1] * scale
            moment = moment + before[2] * scale
            picked = picked + before[3]
        before = (peak, total, moment, picked)
    for k in range(4):
        out[k : k + 1, :] = before[k]


def chunk_kernel(scal, w0, w1, sel, *refs):
    chunk_stats(scal, w0, w1, sel, refs[:-2], refs[-1], refs[-2])


def last_kernel(scal, w0, w1, sel, *refs):
    (near_one, near_two, third), pieces = refs[:3], refs[3:-4]
    stats, extras, hidden, mine = refs[-4:]
    chunk_stats(scal, w0, w1, sel, pieces, hidden, mine)
    left = lax.broadcasted_iota(jnp.int32, (8, 128), 1) < 64
    blocks = {}
    one, two = near_one[:, 128:], near_two[:, :128]
    blocks[0] = near_one[:, :128]
    blocks[1] = jnp.where(left, one, pltpu.roll(two, 64, 1))
    blocks[2] = jnp.where(left, pltpu.roll(one, 64, 1), two)
    blocks[4] = near_two[:, 128:]
    for chunk, pair in ((third, (3, 5)), (mine, (6, 7))):
        for k in range(2):
            blocks[pair[k]] = chunk[:, k * 128 : (k + 1) * 128]
    for relative, block in blocks.items():
        block = jnp.where(scal[5] == 1, pltpu.roll(block, 64, 1), block)
        lanes = pl.ds(pl.multiple_of((relative ^ scal[1]) * 128, 128), 128)
        stats[:, lanes] = block[0:4]
        extras[:, lanes] = block[4:8]


def final_kernel(scal, mine, other, extras, loss_out, logp_out, summary_out, lines):
    first = scal[0] == 0
    logp_c = jnp.where(first, mine[0:1, :], other[0:1, :])
    logp_p = jnp.where(first, other[0:1, :], mine[0:1, :])
    entropy = jnp.where(first, mine[1:2, :], other[1:2, :])
    live = extras[3:4, :]
    loss, weight, ent = token_terms(logp_c, logp_p, entropy, extras[1:2, :], extras[2:3, :], live)
    count = jnp.sum(live, axis=1, keepdims=True)
    lane = lax.broadcasted_iota(jnp.int32, (1, 3), 1)
    summary = jnp.where(lane == 0, jnp.sum(loss, axis=1, keepdims=True), 0.0)
    summary = jnp.where(lane == 1, jnp.sum(weight, axis=1, keepdims=True), summary)
    summary = jnp.where(lane == 2, jnp.sum(ent, axis=1, keepdims=True), summary)
    summary_out[...] = summary / count
    lines[0:1, :] = loss
    lines[1:2, :] = logp_c
    block = lines[:, pl.ds(pl.multiple_of(scal[1] * 128, 128), 128)]
    block = pltpu.roll(block, scal[4], 1)
    loss_out[...] = block[0:1, 0:8]
    logp_out[...] = block[1:2, 0:8]


def merge(a, b):
    peak = jnp.maximum(a[0:1], b[0:1])
    fa, fb = jnp.exp(a[0:1] - peak), jnp.exp(b[0:1] - peak)
    return jnp.concatenate([peak, a[1:3] * fa + b[1:3] * fb, a[3:4] + b[3:4]], axis=0)


def merge_ring(own, others):
    every = [own, *others]
    peak = functools.reduce(jnp.maximum, [v[0:1] for v in every])
    scales = [jnp.exp(v[0:1] - peak) for v in every]
    sums = sum(v[1:3] * f for v, f in zip(every, scales))
    return jnp.concatenate([peak, sums, sum(v[3:4] for v in every)], axis=0)


def token_terms(logp_current, logp_proximal, entropy, advantages, behavior, live):
    ratio = jnp.exp(logp_current - logp_proximal)
    clipped = jnp.clip(ratio, 1.0 - CLIP_EPS, 1.0 + CLIP_EPS)
    surrogate = jnp.maximum(-advantages * ratio, -advantages * clipped)
    weight = jnp.minimum(jnp.exp(logp_proximal - behavior), WEIGHT_CAP)
    return (surrogate * weight * live, weight * live, entropy * live)


def either(first, a, b):
    return jnp.where(first, jnp.concatenate([a, b], axis=0), jnp.concatenate([b, a], axis=0))


def local(
    hidden_current,
    hidden_proximal,
    head_current,
    head_proximal,
    targets,
    loss_mask,
    lengths,
    behavior_logprob,
    advantages,
):
    f32, bf16 = jnp.float32, jnp.bfloat16
    own, depth = hidden_current.shape
    columns = head_current.shape[1]
    tokens = own * 128
    x, y, core, z = [lax.axis_index(a) for a in AXES]
    device = index_of(x, y, core, z)
    first = core == 0
    low = [(v & 1) ^ (v >> 1) for v in (x, y, z)]
    high = [v >> 1 for v in (x, y, z)]
    early_bits, late_bits = [], []
    for dim in range(3):
        pair = (low[dim], high[dim]) if LATE_BIT[0][dim] else (high[dim], low[dim])
        early_bits.append(jnp.where(first, pair[0], pair[1]))
        late_bits.append(jnp.where(first, pair[1], pair[0]))
    early_at = early_bits[0] + 2 * early_bits[1] + 4 * early_bits[2]
    late_at = late_bits[0] + 2 * late_bits[1] + 4 * late_bits[2]
    back = (128 - early_at * 16 - core * 8) % 128
    scal = jnp.stack([core, late_at, device * columns, (device ^ 4) * columns, back, early_bits[2]])
    scal = scal.astype(jnp.int32)

    lines = [targets, loss_mask, jnp.broadcast_to(lengths, (own,)), advantages, behavior_logprob]
    extra = pl.pallas_call(
        extra_kernel,
        out_shape=jax.ShapeDtypeStruct((own, EXTRA), bf16),
        in_specs=[VMEM],
        out_specs=VMEM,
        compiler_params=SMALL,
        name="extra",
    )(jnp.stack([v.astype(f32) for v in lines]))
    keep = jnp.concatenate([jnp.where(first, hidden_current, hidden_proximal), extra], axis=1)
    give = jnp.concatenate([jnp.where(first, hidden_proximal, hidden_current), extra], axis=1)
    block = either(first, keep, swap_core(give))
    heads_c, heads_p, block = lax.optimization_barrier((head_current.T, head_proximal.T, block))
    other_c = swap_core(heads_c)
    other_p = swap_core(heads_p)

    def load(for_c, for_p, limit):
        return pl.pallas_call(
            load_kernel,
            out_shape=jax.ShapeDtypeStruct((columns, depth), bf16),
            in_specs=[SMEM, HBM, HBM],
            out_specs=VMEM,
            scratch_shapes=[pltpu.SemaphoreType.DMA((1,))],
            compiler_params=pltpu.CompilerParams(vmem_limit_bytes=limit * 1024 * 1024),
            cost_estimate=pl.CostEstimate(
                flops=4 * 512 * 2048 * 256, bytes_accessed=4 * columns * depth, transcendentals=0
            ),
            name="load_head",
        )(scal, for_c, for_p)

    w0 = load(heads_c, heads_p, 46)
    got = [swap(block, dims, 0) for dims in (0, 1, (0, 1))]
    w0, *got = lax.optimization_barrier((w0, *got))
    across_x = [either(early_bits[0] == 0, a, b) for a, b in ((block, got[0]), (got[1], got[2]))]
    block = either(early_bits[1] == 0, *across_x)

    weights = [(0, 0, 1.0), (0, 1, 256.0), (0, 2, 65536.0)]
    weights += [(1, 3 + k, 1.0) for k in range(3)]
    weights += [(2, 6 + k, 1.0) for k in range(3)] + [(3, 9, 1.0)]
    table = np.zeros((8, EXTRA), np.float32)
    for a, b, w in weights:
        table[a, b] = w
    sel = jnp.asarray(table, bf16)

    cost = pl.CostEstimate(
        flops=4 * 256 * columns * depth,
        bytes_accessed=4 * columns * depth,
        transcendentals=2 * 256 * columns,
    )
    limit = pltpu.CompilerParams(vmem_limit_bytes=24 * 1024 * 1024)
    hidden = pltpu.VMEM((256, depth), bf16)

    def chunk(*pieces):
        return pl.pallas_call(
            chunk_kernel,
            out_shape=jax.ShapeDtypeStruct((8, 256), f32),
            in_specs=[SMEM] + [VMEM] * (3 + len(pieces)),
            out_specs=VMEM,
            scratch_shapes=[hidden],
            compiler_params=limit,
            cost_estimate=cost,
            name="chunk_stats",
        )(scal, w0, w1, sel, *pieces)

    half = block.shape[0]
    across = swap(block, 2, 0)
    one = [swap(block, dim, 1) for dim in range(2)]
    two = [swap(across, dim, 1) for dim in range(2)]
    group = {4: swap(jnp.concatenate([block, across], axis=0), 2, 1)}
    other_c, other_p, across = lax.optimization_barrier((other_c, other_p, across))
    w1 = load(other_c, other_p, 31)
    w1, two[0], two[1] = lax.optimization_barrier((w1, two[0], two[1]))
    both = [jnp.concatenate([one[dim], two[dim]], axis=0) for dim in range(2)]
    near_one = chunk(block, across, *one)
    near_one, group[4] = lax.optimization_barrier((near_one, group[4]))
    group |= {3: swap(both[1], 0, 1), 5: swap(both[0], 2, 1), 6: swap(group[4], 1, 1)}
    near_two = chunk(*two, group[4])
    near_one, near_two, group[5], group[3] = lax.optimization_barrier(
        (near_one, near_two, group[5], group[3])
    )
    part_one = swap(group[5][:half], 1, 1)
    part_two = swap(group[3][half:], 2, 1)
    third = chunk(group[3], group[5])
    stats, extras = pl.pallas_call(
        last_kernel,
        out_shape=(jax.ShapeDtypeStruct((4, tokens), f32),) * 2,
        in_specs=[SMEM] + [VMEM] * 9,
        out_specs=(VMEM, VMEM),
        scratch_shapes=[hidden, pltpu.VMEM((8, 256), f32)],
        compiler_params=limit,
        cost_estimate=cost,
        name="last_stats",
    )(scal, w0, w1, sel, near_one, near_two, third, group[6], part_one, part_two)

    for dim in range(3):
        stats = merge_ring(stats, [shift(stats, dim, k) for k in (2, 1, 3)])

    lse = stats[0:1] + jnp.log(stats[1:2])
    mine = jnp.concatenate([stats[3:4] - lse, lse - stats[2:3] / stats[1:2]], axis=0)
    other = swap_core(mine).reshape(2, 8, 8, 16).swapaxes(1, 2).reshape(2, tokens)
    loss, logp, summary = pl.pallas_call(
        final_kernel,
        out_shape=(
            jax.ShapeDtypeStruct((1, own), f32),
            jax.ShapeDtypeStruct((1, own), f32),
            jax.ShapeDtypeStruct((1, 3), f32),
        ),
        in_specs=[SMEM, VMEM, VMEM, VMEM],
        out_specs=(VMEM, VMEM, VMEM),
        scratch_shapes=[pltpu.VMEM((8, tokens), f32)],
        compiler_params=SMALL,
        name="final",
    )(scal, mine, other, extras)
    return (loss.reshape(own), logp.reshape(own), summary.reshape(3))


def solution(mesh):
    torus = Mesh(mesh.devices.reshape(4, 4, 2, mesh.shape["vocab"]), AXES)
    spec = P(AXES)
    return jax.shard_map(
        local,
        mesh=torus,
        in_specs=(P(AXES, None), P(AXES, None), P(None, AXES), P(None, AXES)) + (spec,) * 5,
        out_specs=(spec, spec, P()),
        check_vma=False,
    )
```

```python
import functools

import jax
import jax.numpy as jnp
import numpy as np
from jax import lax
from jax.experimental import pallas as pl
from jax.experimental.pallas import tpu as pltpu
from jax.sharding import Mesh
from jax.sharding import PartitionSpec as P

AXES = ("dp_0", "dp_1", "dp_2", "vocab")
SIZES = (4, 4, 2, 4)
CLIP_EPS = 0.2
WEIGHT_CAP = 5.0
EXTRA = 128
LATE_BIT = ((1, 0, 0), (0, 1, 1))


def flip(coordinate, bit):
    return coordinate ^ 1 if bit == 0 else 3 - coordinate


def index_of(x, y, c, z):
    return ((x * 4 + y) * 2 + c) * 4 + z


def swap_pairs(dims, late):
    pairs = []
    for x in range(4):
        for y in range(4):
            for c in range(2):
                for z in range(4):
                    to = [x, y, z]
                    for dim in dims:
                        bit = LATE_BIT[c][dim] if late else 1 - LATE_BIT[c][dim]
                        to[dim] = flip(to[dim], bit)
                    pairs.append((index_of(x, y, c, z), index_of(to[0], to[1], c, to[2])))
    return pairs


def swap(value, dims, late):
    dims = (dims,) if isinstance(dims, int) else dims
    return lax.ppermute(value, AXES, swap_pairs(dims, late))


def shift(value, dim, by):
    pairs = []
    for x in range(4):
        for y in range(4):
            for c in range(2):
                for z in range(4):
                    to = [x, y, z]
                    to[dim] = (to[dim] + by) % 4
                    pairs.append((index_of(x, y, c, z), index_of(to[0], to[1], c, to[2])))
    return lax.ppermute(value, AXES, pairs)


def swap_core(value):
    return lax.ppermute(value, AXES, [(k, k ^ 4) for k in range(128)])


VMEM = pl.BlockSpec(memory_space=pltpu.VMEM)
SMEM = pl.BlockSpec(memory_space=pltpu.SMEM)
HBM = pl.BlockSpec(memory_space=pltpu.HBM)
NT = (((1,), (1,)), ((), ()))
SMALL = pltpu.CompilerParams(vmem_limit_bytes=4 * 1024 * 1024)


def column_of(line):
    rows = lax.broadcasted_iota(jnp.int32, (8, 8), 0)
    lanes = lax.broadcasted_iota(jnp.int32, (8, 8), 1)
    spread = jnp.broadcast_to(line, (8, 8))
    return jnp.sum(jnp.where(rows == lanes, spread, 0.0), axis=1, keepdims=True)


def three_parts(value):
    high = value.astype(jnp.bfloat16).astype(jnp.float32)
    middle = (value - high).astype(jnp.bfloat16).astype(jnp.float32)
    return [high, middle, value - high - middle]


def extra_kernel(lines, extra):
    ids = lines[0:1, :].astype(jnp.int32)
    place = lax.broadcasted_iota(jnp.int32, (1, 8), 1).astype(jnp.float32)
    live = jnp.where((place < lines[2:3, :]) & (lines[1:2, :] == 1.0), 1.0, 0.0)
    values = [v.astype(jnp.float32) for v in (ids & 255, (ids >> 8) & 255, ids >> 16)]
    values += three_parts(lines[3:4, :]) + three_parts(lines[4:5, :]) + [live]
    lane = lax.broadcasted_iota(jnp.int32, extra.shape, 1)
    table = jnp.zeros(extra.shape, jnp.float32)
    for k, value in enumerate(values):
        table = jnp.where(lane == k, column_of(value), table)
    extra[...] = table.astype(jnp.bfloat16)


def load_kernel(scal, for_c, for_p, weights, sem):
    for core, source in enumerate((for_c, for_p)):

        @pl.when(scal[0] == core)
        def _(source=source):
            pltpu.make_async_copy(source, weights, sem.at[0]).start()

    pltpu.make_async_copy(for_c, weights, sem.at[0]).wait()


def chunk_stats(scal, w0, w1, sel, pieces, hidden, out):
    depth = hidden.shape[1]
    at = 0
    for piece in pieces:
        rows = piece.shape[0]
        hidden[at : at + rows, :] = piece[:, :depth]
        out[4:8, at : at + rows] = lax.dot_general(
            sel[...], piece[:, depth:], NT, preferred_element_type=jnp.float32
        )[0:4]
        at += rows
    target = out[4:5, :].astype(jnp.int32)
    before = None
    for h, weights in enumerate((w0, w1)):
        columns = weights.shape[0]
        for first, last in ((0, 512), (512, columns)):
            logits = lax.dot_general(
                weights[first:last, :], hidden[...], NT, preferred_element_type=jnp.float32
            )
            wanted = target - (scal[2 + h] + first)
            peak = jnp.max(logits, axis=0, keepdims=True)
            powers = jnp.exp(logits - peak)
            total = jnp.sum(powers, axis=0, keepdims=True)
            moment = jnp.sum(powers * logits, axis=0, keepdims=True)
            row = lax.broadcasted_iota(jnp.int32, logits.shape, 0)
            picked = jnp.sum(jnp.where(row == wanted, logits, 0.0), axis=0, keepdims=True)
            now = jnp.concatenate([peak, total, moment, picked], axis=0)
            before = now if before is None else merge(before, now)
    out[0:4, :] = before


def chunk_kernel(scal, w0, w1, sel, *refs):
    chunk_stats(scal, w0, w1, sel, refs[:-2], refs[-1], refs[-2])


def last_kernel(scal, w0, w1, sel, *refs):
    (near_one, near_two, third), pieces = refs[:3], refs[3:-4]
    stats, extras, hidden, mine = refs[-4:]
    chunk_stats(scal, w0, w1, sel, pieces, hidden, mine)
    left = lax.broadcasted_iota(jnp.int32, (8, 128), 1) < 64
    blocks = {}
    one, two = near_one[:, 128:], near_two[:, :128]
    blocks[0] = near_one[:, :128]
    blocks[1] = jnp.where(left, one, pltpu.roll(two, 64, 1))
    blocks[2] = jnp.where(left, pltpu.roll(one, 64, 1), two)
    blocks[4] = near_two[:, 128:]
    for chunk, pair in ((third, (3, 5)), (mine, (6, 7))):
        for k in range(2):
            blocks[pair[k]] = chunk[:, k * 128 : (k + 1) * 128]
    for relative, block in blocks.items():
        block = jnp.where(scal[5] == 1, pltpu.roll(block, 64, 1), block)
        lanes = pl.ds(pl.multiple_of((relative ^ scal[1]) * 128, 128), 128)
        stats[:, lanes] = block[0:4]
        extras[:, lanes] = block[4:8]


def final_kernel(scal, mine, other, extras, loss_out, logp_out, summary_out, lines):
    first = scal[0] == 0
    logp_c = jnp.where(first, mine[0:1, :], other[0:1, :])
    logp_p = jnp.where(first, other[0:1, :], mine[0:1, :])
    entropy = jnp.where(first, mine[1:2, :], other[1:2, :])
    live = extras[3:4, :]
    loss, weight, ent = token_terms(logp_c, logp_p, entropy, extras[1:2, :], extras[2:3, :], live)
    count = jnp.sum(live, axis=1, keepdims=True)
    lane = lax.broadcasted_iota(jnp.int32, (1, 3), 1)
    summary = jnp.where(lane == 0, jnp.sum(loss, axis=1, keepdims=True), 0.0)
    summary = jnp.where(lane == 1, jnp.sum(weight, axis=1, keepdims=True), summary)
    summary = jnp.where(lane == 2, jnp.sum(ent, axis=1, keepdims=True), summary)
    summary_out[...] = summary / count
    lines[0:1, :] = loss
    lines[1:2, :] = logp_c
    block = lines[:, pl.ds(pl.multiple_of(scal[1] * 128, 128), 128)]
    block = pltpu.roll(block, scal[4], 1)
    loss_out[...] = block[0:1, 0:8]
    logp_out[...] = block[1:2, 0:8]


def merge(a, b):
    peak = jnp.maximum(a[0:1], b[0:1])
    fa, fb = jnp.exp(a[0:1] - peak), jnp.exp(b[0:1] - peak)
    return jnp.concatenate([peak, a[1:3] * fa + b[1:3] * fb, a[3:4] + b[3:4]], axis=0)


def merge_ring(own, others):
    every = [own, *others]
    peak = functools.reduce(jnp.maximum, [v[0:1] for v in every])
    scales = [jnp.exp(v[0:1] - peak) for v in every]
    sums = sum(v[1:3] * f for v, f in zip(every, scales))
    return jnp.concatenate([peak, sums, sum(v[3:4] for v in every)], axis=0)


def token_terms(logp_current, logp_proximal, entropy, advantages, behavior, live):
    ratio = jnp.exp(logp_current - logp_proximal)
    clipped = jnp.clip(ratio, 1.0 - CLIP_EPS, 1.0 + CLIP_EPS)
    surrogate = jnp.maximum(-advantages * ratio, -advantages * clipped)
    weight = jnp.minimum(jnp.exp(logp_proximal - behavior), WEIGHT_CAP)
    return (surrogate * weight * live, weight * live, entropy * live)


def either(first, a, b):
    return jnp.where(first, jnp.concatenate([a, b], axis=0), jnp.concatenate([b, a], axis=0))


def local(
    hidden_current,
    hidden_proximal,
    head_current,
    head_proximal,
    targets,
    loss_mask,
    lengths,
    behavior_logprob,
    advantages,
):
    f32, bf16 = jnp.float32, jnp.bfloat16
    own, depth = hidden_current.shape
    columns = head_current.shape[1]
    tokens = own * 128
    x, y, core, z = [lax.axis_index(a) for a in AXES]
    device = index_of(x, y, core, z)
    first = core == 0
    low = [(v & 1) ^ (v >> 1) for v in (x, y, z)]
    high = [v >> 1 for v in (x, y, z)]
    early_bits, late_bits = [], []
    for dim in range(3):
        pair = (low[dim], high[dim]) if LATE_BIT[0][dim] else (high[dim], low[dim])
        early_bits.append(jnp.where(first, pair[0], pair[1]))
        late_bits.append(jnp.where(first, pair[1], pair[0]))
    early_at = early_bits[0] + 2 * early_bits[1] + 4 * early_bits[2]
    late_at = late_bits[0] + 2 * late_bits[1] + 4 * late_bits[2]
    back = (128 - early_at * 16 - core * 8) % 128
    scal = jnp.stack([core, late_at, device * columns, (device ^ 4) * columns, back, early_bits[2]])
    scal = scal.astype(jnp.int32)

    lines = [targets, loss_mask, jnp.broadcast_to(lengths, (own,)), advantages, behavior_logprob]
    extra = pl.pallas_call(
        extra_kernel,
        out_shape=jax.ShapeDtypeStruct((own, EXTRA), bf16),
        in_specs=[VMEM],
        out_specs=VMEM,
        compiler_params=SMALL,
        name="extra",
    )(jnp.stack([v.astype(f32) for v in lines]))
    keep = jnp.concatenate([jnp.where(first, hidden_current, hidden_proximal), extra], axis=1)
    give = jnp.concatenate([jnp.where(first, hidden_proximal, hidden_current), extra], axis=1)
    block = either(first, keep, swap_core(give))
    heads_c, heads_p, block = lax.optimization_barrier((head_current.T, head_proximal.T, block))
    other_c = swap_core(heads_c)
    other_p = swap_core(heads_p)

    def load(for_c, for_p, limit):
        return pl.pallas_call(
            load_kernel,
            out_shape=jax.ShapeDtypeStruct((columns, depth), bf16),
            in_specs=[SMEM, HBM, HBM],
            out_specs=VMEM,
            scratch_shapes=[pltpu.SemaphoreType.DMA((1,))],
            compiler_params=pltpu.CompilerParams(vmem_limit_bytes=limit * 1024 * 1024),
            cost_estimate=pl.CostEstimate(
                flops=4 * 512 * 2048 * 256, bytes_accessed=4 * columns * depth, transcendentals=0
            ),
            name="load_head",
        )(scal, for_c, for_p)

    w0 = load(heads_c, heads_p, 46)
    got = [swap(block, dims, 0) for dims in (0, 1, (0, 1))]
    w0, *got = lax.optimization_barrier((w0, *got))
    across_x = [either(early_bits[0] == 0, a, b) for a, b in ((block, got[0]), (got[1], got[2]))]
    block = either(early_bits[1] == 0, *across_x)

    weights = [(0, 0, 1.0), (0, 1, 256.0), (0, 2, 65536.0)]
    weights += [(1, 3 + k, 1.0) for k in range(3)]
    weights += [(2, 6 + k, 1.0) for k in range(3)] + [(3, 9, 1.0)]
    table = np.zeros((8, EXTRA), np.float32)
    for a, b, w in weights:
        table[a, b] = w
    sel = jnp.asarray(table, bf16)

    cost = pl.CostEstimate(
        flops=4 * 256 * columns * depth,
        bytes_accessed=4 * columns * depth,
        transcendentals=2 * 256 * columns,
    )
    limit = pltpu.CompilerParams(vmem_limit_bytes=24 * 1024 * 1024)
    hidden = pltpu.VMEM((256, depth), bf16)

    def chunk(*pieces):
        return pl.pallas_call(
            chunk_kernel,
            out_shape=jax.ShapeDtypeStruct((8, 256), f32),
            in_specs=[SMEM] + [VMEM] * (3 + len(pieces)),
            out_specs=VMEM,
            scratch_shapes=[hidden],
            compiler_params=limit,
            cost_estimate=cost,
            name="chunk_stats",
        )(scal, w0, w1, sel, *pieces)

    half = block.shape[0]
    across = swap(block, 2, 0)
    one = [swap(block, dim, 1) for dim in range(2)]
    two = [swap(across, dim, 1) for dim in range(2)]
    group = {4: swap(jnp.concatenate([block, across], axis=0), 2, 1)}
    other_c, other_p, across = lax.optimization_barrier((other_c, other_p, across))
    w1 = load(other_c, other_p, 31)
    w1, two[0], two[1] = lax.optimization_barrier((w1, two[0], two[1]))
    both = [jnp.concatenate([one[dim], two[dim]], axis=0) for dim in range(2)]
    near_one = chunk(block, across, *one)
    near_one, group[4] = lax.optimization_barrier((near_one, group[4]))
    group |= {3: swap(both[1], 0, 1), 5: swap(both[0], 2, 1), 6: swap(group[4], 1, 1)}
    near_two = chunk(*two, group[4])
    near_one, near_two, group[5], group[3] = lax.optimization_barrier(
        (near_one, near_two, group[5], group[3])
    )
    part_one = swap(group[5][:half], 1, 1)
    part_two = swap(group[3][half:], 2, 1)
    third = chunk(group[3], group[5])
    stats, extras = pl.pallas_call(
        last_kernel,
        out_shape=(jax.ShapeDtypeStruct((4, tokens), f32),) * 2,
        in_specs=[SMEM] + [VMEM] * 9,
        out_specs=(VMEM, VMEM),
        scratch_shapes=[hidden, pltpu.VMEM((8, 256), f32)],
        compiler_params=limit,
        cost_estimate=cost,
        name="last_stats",
    )(scal, w0, w1, sel, near_one, near_two, third, group[6], part_one, part_two)

    for dim in range(3):
        stats = merge_ring(stats, [shift(stats, dim, k) for k in (2, 1, 3)])

    lse = stats[0:1] + jnp.log(stats[1:2])
    mine = jnp.concatenate([stats[3:4] - lse, lse - stats[2:3] / stats[1:2]], axis=0)
    other = swap_core(mine).reshape(2, 8, 8, 16).swapaxes(1, 2).reshape(2, tokens)
    loss, logp, summary = pl.pallas_call(
        final_kernel,
        out_shape=(
            jax.ShapeDtypeStruct((1, own), f32),
            jax.ShapeDtypeStruct((1, own), f32),
            jax.ShapeDtypeStruct((1, 3), f32),
        ),
        in_specs=[SMEM, VMEM, VMEM, VMEM],
        out_specs=(VMEM, VMEM, VMEM),
        scratch_shapes=[pltpu.VMEM((8, tokens), f32)],
        compiler_params=SMALL,
        name="final",
    )(scal, mine, other, extras)
    return (loss.reshape(own), logp.reshape(own), summary.reshape(3))


def solution(mesh):
    torus = Mesh(mesh.devices.reshape(4, 4, 2, mesh.shape["vocab"]), AXES)
    spec = P(AXES)
    return jax.shard_map(
        local,
        mesh=torus,
        in_specs=(P(AXES, None), P(AXES, None), P(None, AXES), P(None, AXES)) + (spec,) * 5,
        out_specs=(spec, spec, P()),
        check_vma=False,
    )
```
